128 devices in a mesh: gx: 16 (over x, y), gy: 4 (over z_hi, core), gz: 2 (over z_lo).
Axes of the slice: x: 4, y: 4, z: 4 (z_hi: 2, z_lo: 2; z = z_hi * 2 + z_lo), core: 2. Of those that a mesh axis runs over, the one named last changes fastest.
Arguments:
- right_side: float32 [256, 256, 1024], P('gx', 'gy', 'gz'), may hold values from -24 to 24
- reaction: float32 [256, 256, 1024], P('gx', 'gy', 'gz'), may hold values from 0.5 to 2
- velocity: float32 [3, 256, 256, 1024], P(None, 'gx', 'gy', 'gz'), may hold values from -0.5 to 0.5
Outputs:
- solution: float32 [256, 256, 1024], P('gx', 'gy', 'gz')
- residual: float32 [256, 256, 1024], P('gx', 'gy', 'gz')
- residual_norm: float32 [], replicated
The draws below stay inside these ranges and needn't reach their ends.
All inputs are finite; a program needn't handle non-finite values.
Results may differ from the reference program's by a relative error of at most 0.00002.
Values sent between devices are 32-bit elements; how exact they have to be, the bound alone decides.
A program may use at most 128 MiB of HBM per device.

```python
import math
import jax
import jax.numpy as jnp

ITERS = 5
NX = 256
NY = 256
NZ = 1024


def draw_right_side(key, part):
    noise_key = jax.random.fold_in(jax.random.fold_in(key, 11), 0)
    ramp = 1.0 + 2.0 * jnp.arange(NX, dtype=jnp.float32)[:, None, None] / max(NX - 1, 1)
    values = ramp * jnp.clip(jax.random.normal(noise_key, (NX, NY, NZ), jnp.float32), -6.0, 6.0)
    return values.astype(jnp.float32)


def block_levels(own_key, extent, shards, least, top_value):
    def one(position, blocks):
        steps = jax.random.uniform(jax.random.fold_in(jax.random.fold_in(own_key, 6), position), (blocks,), jnp.float32, least / len(shards), top_value / len(shards))
        return jnp.repeat(jnp.exp(steps), extent[position] // blocks).reshape((-1,) + (1,) * (len(extent) - position - 1))

    loudness = one(*shards[0])
    for cut in shards[1:]:
        loudness = loudness * one(*cut)
    return loudness


def setup_inputs(seed: int = 0) -> dict:
    arg_keys = jax.random.split(jax.random.key(seed), 4)
    return {
        "right_side": draw_right_side(jax.random.fold_in(arg_keys[3], 71), 0),
        "reaction": jnp.clip(jnp.exp(math.log(2.0) - 1.3862944 * jax.random.uniform(arg_keys[1], (NX, NY, NZ), jnp.float32) ** block_levels(arg_keys[1], (NX, NY, NZ), ((0, 16), (1, 4), (2, 2)), -0.2, 0.2)), 0.5, 2.0),
        "velocity": jnp.clip(jax.random.uniform(arg_keys[2], (3, NX, NY, NZ), jnp.float32, -0.5, 0.5) * block_levels(arg_keys[2], (3, NX, NY, NZ), ((1, 16), (2, 4), (3, 2)), -0.4, 0.0), -0.5, 0.5),
    }


centre = 7.25
half_width = 6.75

def chebyshev_weights(count):
    ratio_value = centre / half_width
    weights = [1.0 / ratio_value]
    for iteration in range(count):
        weights.append(1.0 / (2.0 * ratio_value - weights[-1]))
    return weights

def combine(middle, plus_x, minus_x, plus_y, minus_y, plus_z, minus_z, reaction, velocity):
    beside = (1.0 - velocity[0]) * plus_x + (1.0 + velocity[0]) * minus_x
    beside = beside + (1.0 - velocity[1]) * plus_y + (1.0 + velocity[1]) * minus_y
    beside = beside + (1.0 - velocity[2]) * plus_z + (1.0 + velocity[2]) * minus_z
    return (6.0 + reaction) * middle - beside

def operate(values, reaction, velocity):
    plus_x = jnp.roll(values, -1, 0)
    minus_x = jnp.roll(values, 1, 0)
    padded = jnp.pad(values, ((0, 0), (1, 1), (1, 1)))
    return combine(values, plus_x, minus_x, padded[:, 2:, 1:-1], padded[:, :-2, 1:-1], padded[:, 1:-1, 2:], padded[:, 1:-1, :-2], reaction, velocity)

def reference(right_side, reaction, velocity):
    weights = chebyshev_weights(ITERS)
    solution = jnp.zeros_like(right_side)
    residual = right_side
    direction = right_side / centre
    for iteration in range(ITERS):
        applied = operate(direction, reaction, velocity)
        solution = solution + direction
        residual = residual - applied
        if iteration + 1 < ITERS:
            direction = weights[iteration + 1] * weights[iteration] * direction + 2.0 * weights[iteration + 1] / half_width * residual
    residual_norm = jnp.sqrt(jnp.sum(residual * residual) / (NX * NY * NZ) + 1e-06)
    return (solution, residual, residual_norm)
```

```python
import functools

import jax
import jax.numpy as jnp
from jax import lax
from jax.experimental import pallas as pl
from jax.experimental.pallas import tpu as pltpu
from jax.sharding import PartitionSpec as P

ITERS = 5
centre = 7.25
half_width = 6.75
MESH = pl.DeviceIdType.MESH
F32 = jnp.float32


def chebyshev_weights(count):
    ratio_value = centre / half_width
    weights = [1.0 / ratio_value]
    for iteration in range(count):
        weights.append(1.0 / (2.0 * ratio_value - weights[-1]))
    return weights


NXL, NYL, NT = 16, 64, 4
NJ = NYL // 8
TOP = 8
CELLS = 256 * 256 * 1024


def kernel(
    rhs, rea, vel, sol, res, norm,
    D, V, C, ZS, ZH, G1, G2, G3,
    lf, lr, lc, lv, xs, xr, ys, yr, zs, zr, g1s, g1r, g2s, g2r, g3s, g3r,
):
    gx, gy, gz = lax.axis_index("gx"), lax.axis_index("gy"), lax.axis_index("gz")
    px, py = gx // 4, gx % 4
    yz = gy * 2 + gz
    weights = chebyshev_weights(ITERS)

    def rhs_load(x0, n, t, sem):
        return pltpu.make_async_copy(
            rhs.at[pl.ds(x0, n), :, pl.ds(128 * t, 128)],
            D.at[0, pl.ds(x0 + 1, n), t, pl.ds(TOP, NYL), :],
            sem,
        )

    faces = [rhs_load(x0, 1, t, lf.at[i, t]) for t in range(NT) for i, x0 in enumerate((0, NXL - 1))]
    rest = [rhs_load(1, NXL - 2, t, lr.at[t]) for t in range(NT)]
    coef = [
        pltpu.make_async_copy(rea.at[:, :, pl.ds(128 * t, 128)], C.at[:, t], lc.at[t]) for t in range(NT)
    ] + [
        pltpu.make_async_copy(vel.at[c, :, :, pl.ds(128 * t, 128)], V.at[c, :, t], lv.at[c, t])
        for t in range(NT)
        for c in range(3)
    ]
    for copy in faces + rest + coef:
        copy.start()

    barrier = pltpu.get_barrier_semaphore()
    near = [(gx + 1) % 16, (gx + 15) % 16]
    ring_y = [px * 4 + (py + o) % 4 for o in (1, 2, 3)]
    ring_x = [(gx + 4 * o) % 16 for o in (1, 2, 3)]
    block = [(yz + o) % 8 for o in range(1, 8)]
    peers = [(g, gy, gz) for g in near + ring_y + ring_x] + [(gx, b // 2, b % 2) for b in block]
    for peer in peers:
        pl.semaphore_signal(barrier, inc=1, device_id=peer, device_id_type=MESH)

    zrow = jnp.zeros((1, 128), F32)

    def zero_rows(row):
        def body(x, carry):
            for b in range(2):
                for t in range(NT):
                    D[b, x, t, pl.ds(row, 1), :] = zrow
            return carry

        lax.fori_loop(1, NXL + 1, body, 0)

    @pl.when(gy == 0)
    def _():
        zero_rows(TOP - 1)

    @pl.when(gy == 3)
    def _():
        zero_rows(TOP + NYL)

    for copy in faces:
        copy.wait()
    pl.semaphore_wait(barrier, len(peers))

    x_side = (
        (1, NXL + 1, (gx + 15) % 16),
        (NXL, 0, (gx + 1) % 16),
    )

    def x_copy(buf, side, t):
        src, dst, to = x_side[side]
        return pltpu.make_async_remote_copy(
            src_ref=D.at[buf, src, t, pl.ds(TOP, NYL), :],
            dst_ref=D.at[buf, dst, t, pl.ds(TOP, NYL), :],
            send_sem=xs.at[buf, side, t],
            recv_sem=xr.at[buf, side, t],
            device_id=(to, gy, gz),
            device_id_type=MESH,
        )

    def y_copy(buf, side):
        src = TOP if side == 0 else TOP + NYL - 1
        dst = TOP + NYL if side == 0 else TOP - 1
        to = gy - 1 if side == 0 else gy + 1
        return pltpu.make_async_remote_copy(
            src_ref=D.at[buf, pl.ds(1, NXL), :, pl.ds(src, 1), :],
            dst_ref=D.at[buf, pl.ds(1, NXL), :, pl.ds(dst, 1), :],
            send_sem=ys.at[buf, side],
            recv_sem=yr.at[buf, side],
            device_id=(gx, to, gz),
            device_id_type=MESH,
        )

    def y_each(buf, what):
        if what == "start":
            first, second = gy > 0, gy < 3
        elif what == "recv":
            first, second = gy < 3, gy > 0
        else:
            first, second = gy > 0, gy < 3

        def act(side):
            copy = y_copy(buf, side)
            if what == "start":
                copy.start()
            elif what == "recv":
                copy.wait_recv()
            else:
                copy.wait_send()

        pl.when(first)(lambda: act(0))
        pl.when(second)(lambda: act(1))

    def z_copy(buf):
        return pltpu.make_async_remote_copy(
            src_ref=ZS.at[buf],
            dst_ref=ZH.at[buf],
            send_sem=zs.at[buf],
            recv_sem=zr.at[buf],
            device_id=(gx, gy, 1 - gz),
            device_id_type=MESH,
        )

    lane = lax.broadcasted_iota(jnp.int32, (8, 128), 1)
    first_lane, last_lane = lane == 0, lane == 127
    z_tile = (NT - 1) * (1 - gz)
    low = gz.astype(F32)
    high = 1.0 - low

    def z_pack(buf):
        def body(x, acc):
            for j in range(NJ):
                v = x * NJ + j
                cell = D[buf, x + 1, z_tile, pl.ds(TOP + 8 * j, 8), :]
                cell = pltpu.roll(cell, (v + 1 - gz) % 128, 1)
                acc = jnp.where(lane == v, cell, acc)
            return acc

        ZS[buf] = lax.fori_loop(0, NXL, body, jnp.zeros((8, 128), F32))

    def row_group(step, x, j, tiles, halo, extra=None):
        cur, new = step % 2, (step + 1) % 2
        row = TOP + 8 * j
        lines = pl.ds(8 * j, 8)
        cells, ups, downs = {}, {}, {}

        def cell(t):
            if t not in cells:
                cells[t] = D[cur, x, t, pl.ds(row, 8), :]
            return cells[t]

        def up(t):
            if t not in ups:
                ups[t] = pltpu.roll(cell(t), 127, 1)
            return ups[t]

        def down(t):
            if t not in downs:
                downs[t] = pltpu.roll(cell(t), 1, 1)
            return downs[t]

        if 0 in tiles or NT - 1 in tiles:
            v = (x - 1) * NJ + j
            beyond = pltpu.roll(halo, (127 * (1 - gz) - v + 128) % 128, 1)
        for t in tiles:
            m = cell(t)
            zm = jnp.where(first_lane, down(t - 1) if t else beyond * low, down(t))
            zp = jnp.where(last_lane, up(t + 1) if t < NT - 1 else beyond * high, up(t))
            xm = D[cur, x - 1, t, pl.ds(row, 8), :]
            xp = D[cur, x + 1, t, pl.ds(row, 8), :]
            ym = D[cur, x, t, pl.ds(row - 1, 8), :]
            yp = D[cur, x, t, pl.ds(row + 1, 8), :]
            vx = V[0, x - 1, t, lines, :]
            vy = V[1, x - 1, t, lines, :]
            vz = V[2, x - 1, t, lines, :]
            c = C[x - 1, t, lines, :]
            flow = vx * (xp - xm) + vy * (yp - ym) + vz * (zp - zm)
            beside = ((xp + xm) + (yp + ym)) + (zp + zm)
            applied = (6.0 + c) * m - (beside - flow)
            at = (x - 1, lines, pl.ds(128 * t, 128))
            if step == 0:
                r = m - applied * (1.0 / centre)
                alpha = weights[1] * weights[0] / centre
            else:
                r = res[at] - applied
                alpha = weights[step + 1] * weights[step] if step + 1 < ITERS else 0.0
            res[at] = r
            if step + 1 < ITERS:
                d = alpha * m + (2.0 * weights[step + 1] / half_width) * r
                D[new, x, t, pl.ds(row, 8), :] = d
                if step == 0:
                    sol[at] = m * (1.0 / centre) + d
                else:
                    sol[at] = sol[at] + d
            else:
                extra[(len(extra[-1])) % 4] = extra[len(extra[-1]) % 4] + r * r
                extra[-1].append(0)

    def layers(step, first, last, js, halo):
        def body(x, carry):
            for j in js:
                row_group(step, x, j, range(NT), halo)
            return carry

        lax.fori_loop(first, last, body, 0)

    for t in range(NT):
        for side in range(2):
            x_copy(0, side, t).start()
    for copy in rest:
        copy.wait()
    y_each(0, "start")
    z_pack(0)
    z_copy(0).start()
    for copy in coef:
        copy.wait()

    for step in range(ITERS - 1):
        cur, new = step % 2, (step + 1) % 2
        y_each(cur, "recv")
        z_copy(cur).wait_recv()
        halo = ZH[cur]
        for t in range(NT):
            for side in range(2):
                x_copy(cur, side, t).wait_recv()
            for j in range(NJ):
                for x in (1, NXL):
                    row_group(step, x, j, (t,), halo)
            for side in range(2):
                x_copy(new, side, t).start()
        layers(step, 2, NXL, (0, NJ - 1), halo)
        y_each(new, "start")
        layers(step, 2, NXL, range(1, NJ - 1), halo)
        z_pack(new)
        z_copy(new).start()
        for t in range(NT):
            for side in range(2):
                x_copy(cur, side, t).wait_send()
        y_each(cur, "send")
        z_copy(cur).wait_send()

    step = ITERS - 1
    cur = step % 2
    y_each(cur, "recv")
    z_copy(cur).wait_recv()
    halo = ZH[cur]

    def last_layers(x, sums):
        sums = list(sums) + [[]]
        for j in range(NJ):
            row_group(step, x, j, range(NT), halo, sums)
        return tuple(sums[:4])

    zero = jnp.zeros((8, 128), F32)
    sums = list(lax.fori_loop(2, NXL, last_layers, (zero,) * 4)) + [[]]
    for t in range(NT):
        for side in range(2):
            x_copy(cur, side, t).wait_recv()
        for j in range(NJ):
            for x in (1, NXL):
                row_group(step, x, j, (t,), halo, sums)
    total = (sums[0] + sums[1]) + (sums[2] + sums[3])

    def stage(total, G, send, recv, own, count, place):
        G[own] = total
        copies = [
            pltpu.make_async_remote_copy(
                src_ref=G.at[own],
                dst_ref=G.at[own],
                send_sem=send.at[o - 1],
                recv_sem=recv.at[o - 1],
                device_id=place((own + o) % count),
                device_id_type=MESH,
            )
            for o in range(1, count)
        ]
        for copy in copies:
            copy.start()
        for copy in copies:
            copy.wait_recv()
        total = G[0]
        for i in range(1, count):
            total = total + G[i]
        return total, copies

    total, c1 = stage(total, G1, g1s, g1r, py, 4, lambda p: (px * 4 + p, gy, gz))
    total, c2 = stage(total, G2, g2s, g2r, px, 4, lambda p: (p * 4 + py, gy, gz))
    total, c3 = stage(total, G3, g3s, g3r, yz, 8, lambda p: (gx, p // 2, p % 2))
    whole = jnp.sum(jnp.sum(total, axis=0, keepdims=True), axis=1, keepdims=True)
    norm[...] = jnp.sqrt(whole * (1.0 / CELLS) + 1e-06)
    for t in range(NT):
        for side in range(2):
            x_copy(cur, side, t).wait_send()
    y_each(cur, "send")
    z_copy(cur).wait_send()
    for copy in c1 + c2 + c3:
        copy.wait_send()


def local(right_side, reaction, velocity):
    sem = pltpu.SemaphoreType.DMA
    shape = right_side.shape
    sol, res, norm = pl.pallas_call(
        kernel,
        name="chebyshev",
        out_shape=(pltpu.VMEM(shape, F32), pltpu.VMEM(shape, F32), jax.ShapeDtypeStruct((1, 1), F32)),
        in_specs=[pl.BlockSpec(memory_space=pl.ANY)] * 3,
        out_specs=(pl.BlockSpec(memory_space=pltpu.VMEM),) * 3,
        scratch_shapes=[
            pltpu.VMEM((2, NXL + 2, NT, NYL + 16, 128), F32),
            pltpu.VMEM((3, NXL, NT, NYL, 128), F32),
            pltpu.VMEM((NXL, NT, NYL, 128), F32),
            pltpu.VMEM((2, 8, 128), F32),
            pltpu.VMEM((2, 8, 128), F32),
            pltpu.VMEM((4, 8, 128), F32),
            pltpu.VMEM((4, 8, 128), F32),
            pltpu.VMEM((8, 8, 128), F32),
            sem((2, NT)), sem((NT,)), sem((NT,)), sem((3, NT)),
            sem((2, 2, NT)), sem((2, 2, NT)), sem((2, 2)), sem((2, 2)), sem((2,)), sem((2,)),
            sem((3,)), sem((3,)), sem((3,)), sem((3,)), sem((7,)), sem((7,)),
        ],
        compiler_params=pltpu.CompilerParams(
            collective_id=0, has_side_effects=True, vmem_limit_bytes=24 * 1024 * 1024
        ),
    )(right_side, reaction, velocity)
    return sol, res, norm.reshape(())


def solution(mesh):
    spec = P("gx", "gy", "gz")
    return jax.shard_map(
        local,
        mesh=mesh,
        in_specs=(spec, spec, P(None, "gx", "gy", "gz")),
        out_specs=(spec, spec, P()),
        check_vma=False,
    )
```

```python
import functools

import jax
import jax.numpy as jnp
from jax import lax
from jax.experimental import pallas as pl
from jax.experimental.pallas import tpu as pltpu
from jax.sharding import PartitionSpec as P

ITERS = 5
centre = 7.25
half_width = 6.75
MESH = pl.DeviceIdType.MESH
F32 = jnp.float32


def chebyshev_weights(count):
    ratio_value = centre / half_width
    weights = [1.0 / ratio_value]
    for iteration in range(count):
        weights.append(1.0 / (2.0 * ratio_value - weights[-1]))
    return weights


NXL, NYL, NT = 16, 64, 4
NJ = NYL // 8
TOP = 8
CELLS = 256 * 256 * 1024


def kernel(
    rhs, rea, vel, sol, res, norm,
    D, V, C, ZS, ZH, G1, G2, G3,
    lf, lr, lc, lv, xs, xr, ys, yr, zs, zr, g1s, g1r, g2s, g2r, g3s, g3r,
):
    gx, gy, gz = lax.axis_index("gx"), lax.axis_index("gy"), lax.axis_index("gz")
    px, py = gx // 4, gx % 4
    yz = gy * 2 + gz
    weights = chebyshev_weights(ITERS)

    def rhs_load(x0, n, t, sem):
        return pltpu.make_async_copy(
            rhs.at[pl.ds(x0, n), :, pl.ds(128 * t, 128)],
            D.at[0, pl.ds(x0 + 1, n), t, pl.ds(TOP, NYL), :],
            sem,
        )

    faces = [rhs_load(x0, 1, t, lf.at[i, t]) for t in range(NT) for i, x0 in enumerate((0, NXL - 1))]
    rest = [rhs_load(1, NXL - 2, t, lr.at[t]) for t in range(NT)]
    coef = [
        pltpu.make_async_copy(rea.at[:, :, pl.ds(128 * t, 128)], C.at[:, t], lc.at[t]) for t in range(NT)
    ] + [
        pltpu.make_async_copy(vel.at[c, :, :, pl.ds(128 * t, 128)], V.at[c, :, t], lv.at[c, t])
        for t in range(NT)
        for c in range(3)
    ]
    for copy in faces + rest + coef:
        copy.start()

    barrier = pltpu.get_barrier_semaphore()
    near = [(gx + 1) % 16, (gx + 15) % 16]
    ring_y = [px * 4 + (py + o) % 4 for o in (1, 2, 3)]
    ring_x = [(gx + 4 * o) % 16 for o in (1, 2, 3)]
    block = [(yz + o) % 8 for o in range(1, 8)]
    peers = [(g, gy, gz) for g in near + ring_y + ring_x] + [(gx, b // 2, b % 2) for b in block]
    for peer in peers:
        pl.semaphore_signal(barrier, inc=1, device_id=peer, device_id_type=MESH)

    zrow = jnp.zeros((1, 128), F32)

    def zero_rows(row):
        def body(x, carry):
            for b in range(2):
                for t in range(NT):
                    D[b, x, t, pl.ds(row, 1), :] = zrow
            return carry

        lax.fori_loop(1, NXL + 1, body, 0)

    @pl.when(gy == 0)
    def _():
        zero_rows(TOP - 1)

    @pl.when(gy == 3)
    def _():
        zero_rows(TOP + NYL)

    for copy in faces:
        copy.wait()
    pl.semaphore_wait(barrier, len(peers))

    x_side = (
        (1, NXL + 1, (gx + 15) % 16),
        (NXL, 0, (gx + 1) % 16),
    )

    def x_copy(buf, side, t):
        src, dst, to = x_side[side]
        return pltpu.make_async_remote_copy(
            src_ref=D.at[buf, src, t, pl.ds(TOP, NYL), :],
            dst_ref=D.at[buf, dst, t, pl.ds(TOP, NYL), :],
            send_sem=xs.at[buf, side, t],
            recv_sem=xr.at[buf, side, t],
            device_id=(to, gy, gz),
            device_id_type=MESH,
        )

    def y_copy(buf, side):
        src = TOP if side == 0 else TOP + NYL - 1
        dst = TOP + NYL if side == 0 else TOP - 1
        to = gy - 1 if side == 0 else gy + 1
        return pltpu.make_async_remote_copy(
            src_ref=D.at[buf, pl.ds(1, NXL), :, pl.ds(src, 1), :],
            dst_ref=D.at[buf, pl.ds(1, NXL), :, pl.ds(dst, 1), :],
            send_sem=ys.at[buf, side],
            recv_sem=yr.at[buf, side],
            device_id=(gx, to, gz),
            device_id_type=MESH,
        )

    def y_each(buf, what):
        if what == "start":
            first, second = gy > 0, gy < 3
        elif what == "recv":
            first, second = gy < 3, gy > 0
        else:
            first, second = gy > 0, gy < 3

        def act(side):
            copy = y_copy(buf, side)
            if what == "start":
                copy.start()
            elif what == "recv":
                copy.wait_recv()
            else:
                copy.wait_send()

        pl.when(first)(lambda: act(0))
        pl.when(second)(lambda: act(1))

    def z_copy(buf):
        return pltpu.make_async_remote_copy(
            src_ref=ZS.at[buf],
            dst_ref=ZH.at[buf],
            send_sem=zs.at[buf],
            recv_sem=zr.at[buf],
            device_id=(gx, gy, 1 - gz),
            device_id_type=MESH,
        )

    lane = lax.broadcasted_iota(jnp.int32, (8, 128), 1)
    first_lane, last_lane = lane == 0, lane == 127
    z_tile = (NT - 1) * (1 - gz)
    low = gz.astype(F32)
    high = 1.0 - low

    def z_pack(buf):
        def body(x, acc):
            for j in range(NJ):
                v = x * NJ + j
                cell = D[buf, x + 1, z_tile, pl.ds(TOP + 8 * j, 8), :]
                cell = pltpu.roll(cell, (v + 1 - gz) % 128, 1)
                acc = jnp.where(lane == v, cell, acc)
            return acc

        ZS[buf] = lax.fori_loop(0, NXL, body, jnp.zeros((8, 128), F32))

    def row_group(step, x, j, tiles, halo, extra=None):
        cur, new = step % 2, (step + 1) % 2
        row = TOP + 8 * j
        lines = pl.ds(8 * j, 8)
        cells, ups, downs = {}, {}, {}

        def cell(t):
            if t not in cells:
                cells[t] = D[cur, x, t, pl.ds(row, 8), :]
            return cells[t]

        def up(t):
            if t not in ups:
                ups[t] = pltpu.roll(cell(t), 127, 1)
            return ups[t]

        def down(t):
            if t not in downs:
                downs[t] = pltpu.roll(cell(t), 1, 1)
            return downs[t]

        if 0 in tiles or NT - 1 in tiles:
            v = (x - 1) * NJ + j
            beyond = pltpu.roll(halo, (127 * (1 - gz) - v + 128) % 128, 1)
        for t in tiles:
            m = cell(t)
            zm = jnp.where(first_lane, down(t - 1) if t else beyond * low, down(t))
            zp = jnp.where(last_lane, up(t + 1) if t < NT - 1 else beyond * high, up(t))
            xm = D[cur, x - 1, t, pl.ds(row, 8), :]
            xp = D[cur, x + 1, t, pl.ds(row, 8), :]
            ym = D[cur, x, t, pl.ds(row - 1, 8), :]
            yp = D[cur, x, t, pl.ds(row + 1, 8), :]
            vx = V[0, x - 1, t, lines, :]
            vy = V[1, x - 1, t, lines, :]
            vz = V[2, x - 1, t, lines, :]
            c = C[x - 1, t, lines, :]
            flow = vx * (xp - xm) + vy * (yp - ym) + vz * (zp - zm)
            beside = ((xp + xm) + (yp + ym)) + (zp + zm)
            applied = (6.0 + c) * m - (beside - flow)
            at = (x - 1, lines, pl.ds(128 * t, 128))
            if step == 0:
                r = m - applied * (1.0 / centre)
                alpha = weights[1] * weights[0] / centre
            else:
                r = res[at] - applied
                alpha = weights[step + 1] * weights[step] if step + 1 < ITERS else 0.0
            res[at] = r
            if step + 1 < ITERS:
                d = alpha * m + (2.0 * weights[step + 1] / half_width) * r
                D[new, x, t, pl.ds(row, 8), :] = d
                if step == 0:
                    sol[at] = m * (1.0 / centre) + d
                else:
                    sol[at] = sol[at] + d
            else:
                extra[(len(extra[-1])) % 4] = extra[len(extra[-1]) % 4] + r * r
                extra[-1].append(0)

    def layers(step, first, last, js, halo):
        def body(x, carry):
            for j in js:
                row_group(step, x, j, range(NT), halo)
            return carry

        lax.fori_loop(first, last, body, 0)

    for t in range(NT):
        for side in range(2):
            x_copy(0, side, t).start()
    for copy in rest:
        copy.wait()
    y_each(0, "start")
    z_pack(0)
    z_copy(0).start()
    for copy in coef:
        copy.wait()

    for step in range(ITERS - 1):
        cur, new = step % 2, (step + 1) % 2
        y_each(cur, "recv")
        z_copy(cur).wait_recv()
        halo = ZH[cur]
        for t in range(NT):
            for side in range(2):
                x_copy(cur, side, t).wait_recv()
            for j in range(NJ):
                for x in (1, NXL):
                    row_group(step, x, j, (t,), halo)
            for side in range(2):
                x_copy(new, side, t).start()
        layers(step, 2, NXL, (0, NJ - 1), halo)
        y_each(new, "start")
        layers(step, 2, NXL, range(1, NJ - 1), halo)
        z_pack(new)
        z_copy(new).start()
        for t in range(NT):
            for side in range(2):
                x_copy(cur, side, t).wait_send()
        y_each(cur, "send")
        z_copy(cur).wait_send()

    step = ITERS - 1
    cur = step % 2
    y_each(cur, "recv")
    z_copy(cur).wait_recv()
    halo = ZH[cur]

    def last_layers(x, sums):
        sums = list(sums) + [[]]
        for j in range(NJ):
            row_group(step, x, j, range(NT), halo, sums)
        return tuple(sums[:4])

    zero = jnp.zeros((8, 128), F32)
    sums = list(lax.fori_loop(2, NXL, last_layers, (zero,) * 4)) + [[]]
    for t in range(NT):
        for side in range(2):
            x_copy(cur, side, t).wait_recv()
        for j in range(NJ):
            for x in (1, NXL):
                row_group(step, x, j, (t,), halo, sums)
    total = (sums[0] + sums[1]) + (sums[2] + sums[3])

    def stage(total, G, send, recv, own, count, place):
        G[own] = total
        copies = [
            pltpu.make_async_remote_copy(
                src_ref=G.at[own],
                dst_ref=G.at[own],
                send_sem=send.at[o - 1],
                recv_sem=recv.at[o - 1],
                device_id=place((own + o) % count),
                device_id_type=MESH,
            )
            for o in range(1, count)
        ]
        for copy in copies:
            copy.start()
        for copy in copies:
            copy.wait_recv()
        total = G[0]
        for i in range(1, count):
            total = total + G[i]
        return total, copies

    total, c1 = stage(total, G1, g1s, g1r, py, 4, lambda p: (px * 4 + p, gy, gz))
    total, c2 = stage(total, G2, g2s, g2r, px, 4, lambda p: (p * 4 + py, gy, gz))
    total, c3 = stage(total, G3, g3s, g3r, yz, 8, lambda p: (gx, p // 2, p % 2))
    whole = jnp.sum(jnp.sum(total, axis=0, keepdims=True), axis=1, keepdims=True)
    norm[...] = jnp.sqrt(whole * (1.0 / CELLS) + 1e-06)
    for t in range(NT):
        for side in range(2):
            x_copy(cur, side, t).wait_send()
    y_each(cur, "send")
    z_copy(cur).wait_send()
    for copy in c1 + c2 + c3:
        copy.wait_send()


def local(right_side, reaction, velocity):
    sem = pltpu.SemaphoreType.DMA
    shape = right_side.shape
    sol, res, norm = pl.pallas_call(
        kernel,
        name="chebyshev",
        out_shape=(pltpu.VMEM(shape, F32), pltpu.VMEM(shape, F32), jax.ShapeDtypeStruct((1, 1), F32)),
        in_specs=[pl.BlockSpec(memory_space=pltpu.HBM)] * 3,
        out_specs=(pl.BlockSpec(memory_space=pltpu.VMEM),) * 3,
        scratch_shapes=[
            pltpu.VMEM((2, NXL + 2, NT, NYL + 16, 128), F32),
            pltpu.VMEM((3, NXL, NT, NYL, 128), F32),
            pltpu.VMEM((NXL, NT, NYL, 128), F32),
            pltpu.VMEM((2, 8, 128), F32),
            pltpu.VMEM((2, 8, 128), F32),
            pltpu.VMEM((4, 8, 128), F32),
            pltpu.VMEM((4, 8, 128), F32),
            pltpu.VMEM((8, 8, 128), F32),
            sem((2, NT)), sem((NT,)), sem((NT,)), sem((3, NT)),
            sem((2, 2, NT)), sem((2, 2, NT)), sem((2, 2)), sem((2, 2)), sem((2,)), sem((2,)),
            sem((3,)), sem((3,)), sem((3,)), sem((3,)), sem((7,)), sem((7,)),
        ],
        compiler_params=pltpu.CompilerParams(
            collective_id=0, has_side_effects=True, vmem_limit_bytes=24 * 1024 * 1024
        ),
    )(*[pltpu.with_memory_space_constraint(a, pltpu.HBM) for a in (right_side, reaction, velocity)])
    return sol, res, norm.reshape(())


def solution(mesh):
    spec = P("gx", "gy", "gz")
    return jax.shard_map(
        local,
        mesh=mesh,
        in_specs=(spec, spec, P(None, "gx", "gy", "gz")),
        out_specs=(spec, spec, P()),
        check_vma=False,
    )
```

```python
import functools

import jax
import jax.numpy as jnp
from jax import lax
from jax.experimental import pallas as pl
from jax.experimental.pallas import tpu as pltpu
from jax.sharding import PartitionSpec as P

ITERS = 5
centre = 7.25
half_width = 6.75
MESH = pl.DeviceIdType.MESH
F32 = jnp.float32


def chebyshev_weights(count):
    ratio_value = centre / half_width
    weights = [1.0 / ratio_value]
    for iteration in range(count):
        weights.append(1.0 / (2.0 * ratio_value - weights[-1]))
    return weights


NXL, NYL, NT = 16, 64, 4
NJ = NYL // 8
TOP = 8
CELLS = 256 * 256 * 1024


def kernel(
    rhs, rea, vel, sol, res, norm,
    D0, D1, R, S, V, C, ZS, ZH, G1, G2,
    lf, lr, lc, lv, xs, xr, ys, yr, zs, zr, g1s, g1r, g2s, g2r,
):
    gx, gy, gz = lax.axis_index("gx"), lax.axis_index("gy"), lax.axis_index("gz")
    px, py = gx // 4, gx % 4
    yz = gy * 2 + gz
    weights = chebyshev_weights(ITERS)
    D = (D0, D1)

    def rhs_load(x0, n, t, sem):
        return pltpu.make_async_copy(
            rhs.at[pl.ds(x0, n), :, pl.ds(128 * t, 128)],
            D0.at[pl.ds(x0 + 1, n), t, pl.ds(TOP, NYL), :],
            sem,
        )

    face_loads = [rhs_load(x0, 1, t, lf.at[i, t]) for t in range(NT) for i, x0 in enumerate((0, NXL - 1))]
    rest = [rhs_load(1, NXL - 2, t, lr.at[t]) for t in range(NT)]
    coef = [
        pltpu.make_async_copy(rea.at[:, :, pl.ds(128 * t, 128)], C.at[:, t], lc.at[t]) for t in range(NT)
    ] + [
        pltpu.make_async_copy(vel.at[c, :, :, pl.ds(128 * t, 128)], V.at[c, :, t], lv.at[c, t])
        for t in range(NT)
        for c in range(3)
    ]
    for copy in face_loads + rest + coef:
        copy.start()

    barrier = pltpu.get_barrier_semaphore()
    near = [(gx + 1) % 16, (gx + 15) % 16]
    ring_y = [px * 4 + (py + o) % 4 for o in (1, 2, 3)]
    ring_x = [(gx + 4 * o) % 16 for o in (1, 2, 3)]
    block = [(yz + o) % 8 for o in range(1, 8)]
    peers = [(g, gy, gz) for g in near + ring_y + ring_x] + [(gx, b // 2, b % 2) for b in block]
    for peer in peers:
        pl.semaphore_signal(barrier, inc=1, device_id=peer, device_id_type=MESH)

    zrow = jnp.zeros((1, 128), F32)

    def zero_rows(row):
        def body(x, carry):
            for b in range(2):
                for t in range(NT):
                    D[b][x, t, pl.ds(row, 1), :] = zrow
            return carry

        lax.fori_loop(1, NXL + 1, body, 0)

    @pl.when(gy == 0)
    def _():
        zero_rows(TOP - 1)

    @pl.when(gy == 3)
    def _():
        zero_rows(TOP + NYL)

    for copy in face_loads:
        copy.wait()
    pl.semaphore_wait(barrier, len(peers))

    x_side = (
        (1, NXL + 1, (gx + 15) % 16),
        (NXL, 0, (gx + 1) % 16),
    )

    def x_copy(buf, side, t):
        src, dst, to = x_side[side]
        return pltpu.make_async_remote_copy(
            src_ref=D[buf].at[src, t, pl.ds(TOP, NYL), :],
            dst_ref=D[buf].at[dst, t, pl.ds(TOP, NYL), :],
            send_sem=xs.at[buf, side, t],
            recv_sem=xr.at[buf, side, t],
            device_id=(to, gy, gz),
            device_id_type=MESH,
        )

    y_side = (
        (TOP, TOP + NYL, gy - 1, gy > 0, gy < 3),
        (TOP + NYL - 1, TOP - 1, gy + 1, gy < 3, gy > 0),
    )

    def y_copies(buf, side, chunk):
        src, dst, to, _, _ = y_side[side]
        if chunk == 0:
            parts = [(pl.ds(2, NXL - 2), slice(None), 0)]
        else:
            parts = [(pl.ds(x, 1), pl.ds(chunk - 1, 1), i) for i, x in enumerate((1, NXL))]
        return [
            pltpu.make_async_remote_copy(
                src_ref=D[buf].at[xs_, ts_, pl.ds(src, 1), :],
                dst_ref=D[buf].at[xs_, ts_, pl.ds(dst, 1), :],
                send_sem=ys.at[buf, side, chunk, i],
                recv_sem=yr.at[buf, side, chunk, i],
                device_id=(gx, to, gz),
                device_id_type=MESH,
            )
            for xs_, ts_, i in parts
        ]

    def y_each(buf, chunk, what):
        def act(side):
            for copy in y_copies(buf, side, chunk):
                getattr(copy, what)()

        for side in range(2):
            sends, gets = y_side[side][3:]
            pl.when(gets if what == "wait_recv" else sends)(functools.partial(act, side))

    def z_copy(buf, part):
        return pltpu.make_async_remote_copy(
            src_ref=ZS.at[buf, part],
            dst_ref=ZH.at[buf, part],
            send_sem=zs.at[buf, part],
            recv_sem=zr.at[buf, part],
            device_id=(gx, gy, 1 - gz),
            device_id_type=MESH,
        )

    lane = lax.broadcasted_iota(jnp.int32, (8, 128), 1)
    first_lane, last_lane = lane == 0, lane == 127
    z_tile = (NT - 1) * (1 - gz)
    low = gz.astype(F32)
    high = 1.0 - low

    def z_pack(buf, part):
        def add(x, acc):
            for j in range(NJ):
                v = (x - 1) * NJ + j
                cell = D[buf][x, z_tile, pl.ds(TOP + 8 * j, 8), :]
                cell = pltpu.roll(cell, (v + 1 - gz) & 127, 1)
                acc = jnp.where(lane == v, cell, acc)
            return acc

        def body(i, accs):
            return tuple(add(2 + 7 * a + i, acc) for a, acc in enumerate(accs))

        zero = jnp.zeros((8, 128), F32)
        if part == 0:
            first, second = lax.fori_loop(0, (NXL - 2) // 2, body, (zero, zero))
            ZS[buf, 0] = first + second
        else:
            ZS[buf, 1] = add(1, zero) + add(NXL, zero)

    def row_group(step, x, j, tiles, halo, sums=None):
        now, new = D[step % 2], D[(step + 1) % 2]
        row = TOP + 8 * j
        lines = pl.ds(8 * j, 8)
        cells, ups, downs, stores = {}, {}, {}, []

        def cell(t):
            if t not in cells:
                cells[t] = now[x, t, pl.ds(row, 8), :]
            return cells[t]

        def up(t):
            if t not in ups:
                ups[t] = pltpu.roll(cell(t), 127, 1)
            return ups[t]

        def down(t):
            if t not in downs:
                downs[t] = pltpu.roll(cell(t), 1, 1)
            return downs[t]

        if 0 in tiles or NT - 1 in tiles:
            v = (x - 1) * NJ + j
            beyond = pltpu.roll(halo, (127 * (1 - gz) - v) & 127, 1)
        for t in tiles:
            m = cell(t)
            zm = jnp.where(first_lane, down(t - 1) if t else beyond * low, down(t))
            zp = jnp.where(last_lane, up(t + 1) if t < NT - 1 else beyond * high, up(t))
            xm = now[x - 1, t, pl.ds(row, 8), :]
            xp = now[x + 1, t, pl.ds(row, 8), :]
            ym = now[x, t, pl.ds(row - 1, 8), :]
            yp = now[x, t, pl.ds(row + 1, 8), :]
            at = (x - 1, t, lines, slice(None))
            vx, vy, vz = (V[(c,) + at] for c in range(3))
            flow = vx * (xp - xm) + vy * (yp - ym) + vz * (zp - zm)
            beside = ((xp + xm) + (yp + ym)) + (zp + zm)
            applied = (6.0 + C[at]) * m - (beside - flow)
            out = (x - 1, lines, pl.ds(128 * t, 128))
            if step == 0:
                r = m - applied * (1.0 / centre)
                alpha = weights[1] * weights[0] / centre
            else:
                r = R[at] - applied
                alpha = weights[step + 1] * weights[step] if step + 1 < ITERS else 0.0
            if step + 1 < ITERS:
                d = alpha * m + (2.0 * weights[step + 1] / half_width) * r
                s = (m * (1.0 / centre) if step == 0 else S[at]) + d
                stores.append((R, at, r))
                stores.append((new, (x, t, pl.ds(row, 8), slice(None)), d))
                stores.append((S, at, s) if step + 2 < ITERS else (sol, out, s))
            else:
                stores.append((res, out, r))
                sums[t] = sums[t] + r * r
        return stores

    def groups(step, items, halo, sums=None):
        held = []
        for x, j, tiles in items:
            stores = row_group(step, x, j, tiles, halo, sums)
            for ref, at, value in held:
                ref[at] = value
            held = stores
        for ref, at, value in held:
            ref[at] = value

    def layers(step, js, halo, many):
        def body(i, carry):
            groups(step, [(2 + i * many + k, j, range(NT)) for k in range(many) for j in js], halo)
            return carry

        lax.fori_loop(0, (NXL - 2) // many, body, 0)

    def faces(step, t, sums=None):
        groups(step, [(x, j, (t,)) for j in range(NJ) for x in (1, NXL)], ZH[step % 2, 1], sums)

    for t in range(NT):
        for side in range(2):
            x_copy(0, side, t).start()
    for copy in rest:
        copy.wait()
    for chunk in range(NT + 1):
        y_each(0, chunk, "start")
    for part in range(2):
        z_pack(0, part)
        z_copy(0, part).start()
    for copy in coef:
        copy.wait()

    for step in range(ITERS - 1):
        cur, new = step % 2, (step + 1) % 2
        y_each(cur, 0, "wait_recv")
        z_copy(cur, 0).wait_recv()
        halo = ZH[cur, 0]
        layers(step, (0, NJ - 1), halo, 7)
        y_each(new, 0, "start")
        layers(step, range(1, NJ - 1), halo, 2)
        z_pack(new, 0)
        z_copy(new, 0).start()
        z_copy(cur, 1).wait_recv()
        for t in range(NT):
            for side in range(2):
                x_copy(cur, side, t).wait_recv()
            y_each(cur, t + 1, "wait_recv")
            faces(step, t)
            for side in range(2):
                x_copy(new, side, t).start()
            y_each(new, t + 1, "start")
        z_pack(new, 1)
        z_copy(new, 1).start()
        for t in range(NT):
            for side in range(2):
                x_copy(cur, side, t).wait_send()
        for chunk in range(NT + 1):
            y_each(cur, chunk, "wait_send")
        for part in range(2):
            z_copy(cur, part).wait_send()

    step = ITERS - 1
    cur = step % 2
    y_each(cur, 0, "wait_recv")
    z_copy(cur, 0).wait_recv()
    halo = ZH[cur, 0]

    def last_layers(i, sums):
        sums = list(sums)
        groups(step, [(2 + 2 * i + k, j, range(NT)) for k in range(2) for j in range(NJ)], halo, sums)
        return tuple(sums)

    zero = jnp.zeros((8, 128), F32)
    sums = list(lax.fori_loop(0, (NXL - 2) // 2, last_layers, (zero,) * NT))
    z_copy(cur, 1).wait_recv()
    for t in range(NT):
        for side in range(2):
            x_copy(cur, side, t).wait_recv()
        y_each(cur, t + 1, "wait_recv")
        faces(step, t, sums)
    total = (sums[0] + sums[1]) + (sums[2] + sums[3])

    def stage(total, G, send, recv, own, count, place):
        G[own] = total
        copies = [
            pltpu.make_async_remote_copy(
                src_ref=G.at[own],
                dst_ref=G.at[own],
                send_sem=send.at[o - 1],
                recv_sem=recv.at[o - 1],
                device_id=place((own + o) % count),
                device_id_type=MESH,
            )
            for o in range(1, count)
        ]
        for copy in copies:
            copy.start()
        for copy in copies:
            copy.wait_recv()
        total = G[0]
        for i in range(1, count):
            total = total + G[i]
        return total, copies

    total, c1 = stage(total, G1, g1s, g1r, gx, 16, lambda p: (p, gy, gz))
    total, c2 = stage(total, G2, g2s, g2r, yz, 8, lambda p: (gx, p // 2, p % 2))
    whole = jnp.sum(jnp.sum(total, axis=0, keepdims=True), axis=1, keepdims=True)
    norm[...] = jnp.sqrt(whole * (1.0 / CELLS) + 1e-06)
    for t in range(NT):
        for side in range(2):
            x_copy(cur, side, t).wait_send()
    for chunk in range(NT + 1):
        y_each(cur, chunk, "wait_send")
    for part in range(2):
        z_copy(cur, part).wait_send()
    for copy in c1 + c2:
        copy.wait_send()


def local(right_side, reaction, velocity):
    sem = pltpu.SemaphoreType.DMA
    shape = right_side.shape
    sol, res, norm = pl.pallas_call(
        kernel,
        name="chebyshev",
        out_shape=(pltpu.VMEM(shape, F32), pltpu.VMEM(shape, F32), jax.ShapeDtypeStruct((1, 1), F32)),
        in_specs=[pl.BlockSpec(memory_space=pltpu.HBM)] * 3,
        out_specs=(pl.BlockSpec(memory_space=pltpu.VMEM),) * 3,
        scratch_shapes=[
            pltpu.VMEM((NXL + 2, NT, NYL + 16, 128), F32),
            pltpu.VMEM((NXL + 2, NT, NYL + 16, 128), F32),
            pltpu.VMEM((NXL, NT, NYL, 128), F32),
            pltpu.VMEM((NXL, NT, NYL, 128), F32),
            pltpu.VMEM((3, NXL, NT, NYL, 128), F32),
            pltpu.VMEM((NXL, NT, NYL, 128), F32),
            pltpu.VMEM((2, 2, 8, 128), F32),
            pltpu.VMEM((2, 2, 8, 128), F32),
            pltpu.VMEM((16, 8, 128), F32),
            pltpu.VMEM((8, 8, 128), F32),
            sem((2, NT)), sem((NT,)), sem((NT,)), sem((3, NT)),
            sem((2, 2, NT)), sem((2, 2, NT)), sem((2, 2, NT + 1, 2)), sem((2, 2, NT + 1, 2)),
            sem((2, 2)), sem((2, 2)), sem((15,)), sem((15,)), sem((7,)), sem((7,)),
        ],
        compiler_params=pltpu.CompilerParams(
            collective_id=0, has_side_effects=True, vmem_limit_bytes=24 * 1024 * 1024
        ),
    )(*[pltpu.with_memory_space_constraint(a, pltpu.HBM) for a in (right_side, reaction, velocity)])
    return sol, res, norm.reshape(())


def solution(mesh):
    spec = P("gx", "gy", "gz")
    return jax.shard_map(
        local,
        mesh=mesh,
        in_specs=(spec, spec, P(None, "gx", "gy", "gz")),
        out_specs=(spec, spec, P()),
        check_vma=False,
    )
```

```python
import functools

import jax
import jax.numpy as jnp
from jax import lax
from jax.experimental import pallas as pl
from jax.experimental.pallas import tpu as pltpu
from jax.sharding import PartitionSpec as P

ITERS = 5
centre = 7.25
half_width = 6.75
MESH = pl.DeviceIdType.MESH
F32 = jnp.float32


def chebyshev_weights(count):
    ratio_value = centre / half_width
    weights = [1.0 / ratio_value]
    for iteration in range(count):
        weights.append(1.0 / (2.0 * ratio_value - weights[-1]))
    return weights


NXL, NYL, NT = 16, 64, 4
NJ = NYL // 8
TOP = 8
NH = 2
CELLS = 256 * 256 * 1024
SLABS = ((1, 6), (7, 4), (11, 4), (0, 1), (15, 1))


def kernel(
    rhs, rea, vel, sol, res, norm,
    D0, D1, R, S, V, C, ZS, ZH, G1, G2,
    lf, lr, lc, lv, xs, xr, ys, yr, zs, zr, g1s, g1r, g2s, g2r,
):
    gx, gy, gz = lax.axis_index("gx"), lax.axis_index("gy"), lax.axis_index("gz")
    px, py = gx // 4, gx % 4
    yz = gy * 2 + gz
    weights = chebyshev_weights(ITERS)
    D = (D0, D1)

    barrier = pltpu.get_barrier_semaphore()
    near = [(gx + 1) % 16, (gx + 15) % 16]
    ring_y = [px * 4 + (py + o) % 4 for o in (1, 2, 3)]
    ring_x = [(gx + 4 * o) % 16 for o in (1, 2, 3)]
    block = [(yz + o) % 8 for o in range(1, 8)]
    peers = [(g, gy, gz) for g in near + ring_y + ring_x] + [(gx, b // 2, b % 2) for b in block]
    for peer in peers:
        pl.semaphore_signal(barrier, inc=1, device_id=peer, device_id_type=MESH)

    def rhs_load(x0, n, t, sem):
        return pltpu.make_async_copy(
            rhs.at[pl.ds(x0, n), :, pl.ds(128 * t, 128)],
            D0.at[pl.ds(x0 + 1, n), t, pl.ds(TOP, NYL), :],
            sem,
        )

    face_loads = [rhs_load(x0, 1, t, lf.at[i, t]) for t in range(NT) for i, x0 in enumerate((0, NXL - 1))]
    rest = [rhs_load(1, NXL - 2, t, lr.at[t]) for t in range(NT)]

    def coef_load(x0, n, i):
        out = []
        for t in range(NT):
            lanes = pl.ds(128 * t, 128)
            out.append(pltpu.make_async_copy(rea.at[pl.ds(x0, n), :, lanes], C.at[pl.ds(x0, n), t], lc.at[i, t]))
            out += [
                pltpu.make_async_copy(
                    vel.at[c, pl.ds(x0, n), :, lanes], V.at[c, pl.ds(x0, n), t], lv.at[i, c, t]
                )
                for c in range(3)
            ]
        return out

    slabs = [coef_load(x0, n, i) for i, (x0, n) in enumerate(SLABS)]
    for copy in face_loads + rest + sum(slabs, []):
        copy.start()

    zrow = jnp.zeros((1, 128), F32)

    def zero_rows(row):
        def body(x, carry):
            for b in range(2):
                for t in range(NT):
                    D[b][x, t, pl.ds(row, 1), :] = zrow
            return carry

        lax.fori_loop(1, NXL + 1, body, 0)

    @pl.when(gy == 0)
    def _():
        zero_rows(TOP - 1)

    @pl.when(gy == 3)
    def _():
        zero_rows(TOP + NYL)

    for copy in face_loads:
        copy.wait()
    pl.semaphore_wait(barrier, len(peers))

    x_side = (
        (1, NXL + 1, (gx + 15) % 16),
        (NXL, 0, (gx + 1) % 16),
    )

    def tile(t):
        return t + gz * (NT - 1 - 2 * t)

    def x_copy(buf, side, t, h):
        src, dst, to = x_side[side]
        rows = pl.ds(TOP + h * (NYL // NH), NYL // NH)
        return pltpu.make_async_remote_copy(
            src_ref=D[buf].at[src, tile(t), rows, :],
            dst_ref=D[buf].at[dst, tile(t), rows, :],
            send_sem=xs.at[buf, side, t, h],
            recv_sem=xr.at[buf, side, t, h],
            device_id=(to, gy, gz),
            device_id_type=MESH,
        )

    def x_each(buf, t, h, what):
        for side in range(2):
            getattr(x_copy(buf, side, t, h), what)()

    chunks = [(t, h) for t in range(NT) for h in range(NH)]

    y_side = (
        (TOP, TOP + NYL, gy - 1, gy > 0, gy < 3),
        (TOP + NYL - 1, TOP - 1, gy + 1, gy < 3, gy > 0),
    )

    def y_copies(buf, side, chunk):
        src, dst, to, _, _ = y_side[side]
        if chunk == 0:
            parts = [(pl.ds(2, NXL - 2), slice(None), 0)]
        else:
            parts = [(pl.ds(x, 1), pl.ds(tile(chunk - 1), 1), i) for i, x in enumerate((1, NXL))]
        return [
            pltpu.make_async_remote_copy(
                src_ref=D[buf].at[xs_, ts_, pl.ds(src, 1), :],
                dst_ref=D[buf].at[xs_, ts_, pl.ds(dst, 1), :],
                send_sem=ys.at[buf, side, chunk, i],
                recv_sem=yr.at[buf, side, chunk, i],
                device_id=(gx, to, gz),
                device_id_type=MESH,
            )
            for xs_, ts_, i in parts
        ]

    def y_each(buf, chunk, what, which=(0, 1)):
        def act(side):
            for copy in y_copies(buf, side, chunk):
                getattr(copy, what)()

        for side in which:
            sends, gets = y_side[side][3:]
            pl.when(gets if what == "wait_recv" else sends)(functools.partial(act, side))

    def z_copy(buf, part):
        return pltpu.make_async_remote_copy(
            src_ref=ZS.at[buf, part],
            dst_ref=ZH.at[buf, part],
            send_sem=zs.at[buf, part],
            recv_sem=zr.at[buf, part],
            device_id=(gx, gy, 1 - gz),
            device_id_type=MESH,
        )

    lane = lax.broadcasted_iota(jnp.int32, (8, 128), 1)
    first_lane, last_lane = lane == 0, lane == 127
    z_tile = (NT - 1) * (1 - gz)
    low = gz.astype(F32)
    high = 1.0 - low

    def z_pack(buf, part):
        def add(x, acc):
            for j in range(NJ):
                v = (x - 1) * NJ + j
                cell = D[buf][x, z_tile, pl.ds(TOP + 8 * j, 8), :]
                cell = pltpu.roll(cell, (v + 1 - gz) & 127, 1)
                acc = jnp.where(lane == v, cell, acc)
            return acc

        def body(i, accs):
            return tuple(add(2 + 7 * a + i, acc) for a, acc in enumerate(accs))

        zero = jnp.zeros((8, 128), F32)
        if part == 0:
            first, second = lax.fori_loop(0, (NXL - 2) // 2, body, (zero, zero))
            ZS[buf, 0] = first + second
        else:
            ZS[buf, 1] = add(1, zero) + add(NXL, zero)

    def row_group(step, x, j, tiles, halo, sums=None):
        now = D[step % 2]
        row = TOP + 8 * j
        lines = pl.ds(8 * j, 8)
        cells, ups, downs, stores = {}, {}, {}, []

        def cell(t):
            if t not in cells:
                cells[t] = now[x, t, pl.ds(row, 8), :]
            return cells[t]

        def up(t):
            if t not in ups:
                ups[t] = pltpu.roll(cell(t), 127, 1)
            return ups[t]

        def down(t):
            if t not in downs:
                downs[t] = pltpu.roll(cell(t), 1, 1)
            return downs[t]

        if 0 in tiles or NT - 1 in tiles:
            v = (x - 1) * NJ + j
            beyond = pltpu.roll(halo, (127 * (1 - gz) - v) & 127, 1)
        for t in tiles:
            m = cell(t)
            zm = jnp.where(first_lane, down(t - 1) if t else beyond * low, down(t))
            zp = jnp.where(last_lane, up(t + 1) if t < NT - 1 else beyond * high, up(t))
            stores += cell_step(step, x, t, row, lines, m, zm, zp, sums, t)
        return stores

    def face_group(step, x, j, t, halo, sums=None):
        now = D[step % 2]
        row = TOP + 8 * j
        lines, rows = pl.ds(8 * j, 8), pl.ds(row, 8)
        at_t = tile(t)
        m = now[x, at_t, rows, :]
        down, up = pltpu.roll(m, 1, 1), pltpu.roll(m, 127, 1)
        before = pltpu.roll(now[x, jnp.maximum(at_t - 1, 0), rows, :], 1, 1)
        after = pltpu.roll(now[x, jnp.minimum(at_t + 1, NT - 1), rows, :], 127, 1)
        if t == 0:
            before, after = before * low, after * high
        if t == NT - 1:
            v = (x - 1) * NJ + j
            beyond = pltpu.roll(halo, (127 * (1 - gz) - v) & 127, 1)
            before = before * high + beyond * low
            after = after * low + beyond * high
        zm = jnp.where(first_lane, before, down)
        zp = jnp.where(last_lane, after, up)
        return cell_step(step, x, at_t, row, lines, m, zm, zp, sums, t)

    def cell_step(step, x, t, row, lines, m, zm, zp, sums, slot):
        now, new = D[step % 2], D[(step + 1) % 2]
        xm = now[x - 1, t, pl.ds(row, 8), :]
        xp = now[x + 1, t, pl.ds(row, 8), :]
        ym = now[x, t, pl.ds(row - 1, 8), :]
        yp = now[x, t, pl.ds(row + 1, 8), :]
        at = (x - 1, t, lines, slice(None))
        vx, vy, vz = (V[(c,) + at] for c in range(3))
        flow = vx * (xp - xm) + vy * (yp - ym) + vz * (zp - zm)
        beside = ((xp + xm) + (yp + ym)) + (zp + zm)
        applied = (6.0 + C[at]) * m - (beside - flow)
        lanes = pl.ds(128 * t if isinstance(t, int) else pl.multiple_of(128 * t, 128), 128)
        out = (x - 1, lines, lanes)
        if step == 0:
            r = m - applied * (1.0 / centre)
            alpha = weights[1] * weights[0] / centre
        else:
            r = R[at] - applied
            alpha = weights[step + 1] * weights[step] if step + 1 < ITERS else 0.0
        if step + 1 == ITERS:
            sums[slot] = sums[slot] + r * r
            return [(res, out, r)]
        d = alpha * m + (2.0 * weights[step + 1] / half_width) * r
        s = (m * (1.0 / centre) if step == 0 else S[at]) + d
        return [
            (R, at, r),
            (new, (x, t, pl.ds(row, 8), slice(None)), d),
            (S, at, s) if step + 2 < ITERS else (sol, out, s),
        ]

    def late(parts):
        held = []
        for part in parts:
            stores = part()
            for ref, at, value in held:
                ref[at] = value
            held = stores
        for ref, at, value in held:
            ref[at] = value

    def groups(step, items, halo, sums=None):
        late([functools.partial(row_group, step, x, j, range(NT), halo, sums) for x, j in items])

    def layers(step, first, count, js, halo, many):
        def body(i, carry):
            groups(step, [(first + i * many + k, j) for k in range(many) for j in js], halo)
            return carry

        lax.fori_loop(0, count // many, body, 0)

    def faces(step, t, h, sums=None):
        js = range(h * (NJ // NH), (h + 1) * (NJ // NH))
        halo = ZH[step % 2, 1]
        late([functools.partial(face_group, step, x, j, t, halo, sums) for j in js for x in (1, NXL)])

    for t, h in chunks:
        x_each(0, t, h, "start")
    for copy in rest:
        copy.wait()
    for chunk in range(NT + 1):
        y_each(0, chunk, "start")
    for part in range(2):
        z_pack(0, part)
        z_copy(0, part).start()

    for step in range(ITERS):
        cur, new, more = step % 2, (step + 1) % 2, step + 1 < ITERS
        y_each(cur, 0, "wait_recv")
        z_copy(cur, 0).wait_recv()
        halo = ZH[cur, 0]
        sums = None
        if step == 0:
            for (x0, n), slab in list(zip(SLABS, slabs))[:3]:
                for copy in slab:
                    copy.wait()
                layers(step, x0 + 1, n, range(NJ), halo, 2)
            y_each(new, 0, "start")
        elif more:
            layers(step, 2, NXL - 2, (0, NJ - 1), halo, 7)
            y_each(new, 0, "start")
            layers(step, 2, NXL - 2, range(1, NJ - 1), halo, 2)
        else:

            def last_layers(i, sums):
                sums = list(sums)
                groups(step, [(2 + 2 * i + k, j) for k in range(2) for j in range(NJ)], halo, sums)
                return tuple(sums)

            zero = jnp.zeros((8, 128), F32)
            sums = list(lax.fori_loop(0, (NXL - 2) // 2, last_layers, (zero,) * NT))
        if more:
            z_pack(new, 0)
            z_copy(new, 0).start()
        if step == 0:
            for copy in slabs[3] + slabs[4]:
                copy.wait()
        for t, h in chunks:
            x_each(cur, t, h, "wait_recv")
            if h == 0:
                y_each(cur, t + 1, "wait_recv", (1,))
            if h == NH - 1:
                y_each(cur, t + 1, "wait_recv", (0,))
            if (t, h) == (NT - 1, 0):
                z_copy(cur, 1).wait_recv()
            faces(step, t, h, sums)
            if more:
                x_each(new, t, h, "start")
                if h == 0:
                    y_each(new, t + 1, "start", (0,))
                if h == NH - 1:
                    y_each(new, t + 1, "start", (1,))
        if more:
            z_pack(new, 1)
            z_copy(new, 1).start()
            for t, h in chunks:
                x_each(cur, t, h, "wait_send")
            for chunk in range(NT + 1):
                y_each(cur, chunk, "wait_send")
            for part in range(2):
                z_copy(cur, part).wait_send()
    total = jnp.sum((sums[0] + sums[1]) + (sums[2] + sums[3]), axis=0, keepdims=True)

    def stage(total, G, send, recv, own, count, place):
        G[own, pl.ds(0, 1), :] = total
        copies = [
            pltpu.make_async_remote_copy(
                src_ref=G.at[own, pl.ds(0, 1), :],
                dst_ref=G.at[own, pl.ds(0, 1), :],
                send_sem=send.at[o - 1],
                recv_sem=recv.at[o - 1],
                device_id=place((own + o) % count),
                device_id_type=MESH,
            )
            for o in range(1, count)
        ]
        for copy in copies:
            copy.start()
        for copy in copies:
            copy.wait_recv()
        parts = [G[i, pl.ds(0, 1), :] for i in range(count)]
        while len(parts) > 1:
            parts = [a + b for a, b in zip(parts[::2], parts[1::2])]
        return parts[0], copies

    total, c1 = stage(total, G1, g1s, g1r, gx, 16, lambda p: (p, gy, gz))
    total, c2 = stage(total, G2, g2s, g2r, yz, 8, lambda p: (gx, p // 2, p % 2))
    whole = jnp.sum(total, axis=1, keepdims=True)
    norm[...] = jnp.sqrt(whole * (1.0 / CELLS) + 1e-06)
    cur = (ITERS - 1) % 2
    for t, h in chunks:
        x_each(cur, t, h, "wait_send")
    for chunk in range(NT + 1):
        y_each(cur, chunk, "wait_send")
    for part in range(2):
        z_copy(cur, part).wait_send()
    for copy in c1 + c2:
        copy.wait_send()


def local(right_side, reaction, velocity):
    sem = pltpu.SemaphoreType.DMA
    shape = right_side.shape
    sol, res, norm = pl.pallas_call(
        kernel,
        name="chebyshev",
        out_shape=(pltpu.VMEM(shape, F32), pltpu.VMEM(shape, F32), jax.ShapeDtypeStruct((1, 1), F32)),
        in_specs=[pl.BlockSpec(memory_space=pltpu.HBM)] * 3,
        out_specs=(pl.BlockSpec(memory_space=pltpu.VMEM),) * 3,
        scratch_shapes=[
            pltpu.VMEM((NXL + 2, NT, NYL + 16, 128), F32),
            pltpu.VMEM((NXL + 2, NT, NYL + 16, 128), F32),
            pltpu.VMEM((NXL, NT, NYL, 128), F32),
            pltpu.VMEM((NXL, NT, NYL, 128), F32),
            pltpu.VMEM((3, NXL, NT, NYL, 128), F32),
            pltpu.VMEM((NXL, NT, NYL, 128), F32),
            pltpu.VMEM((2, 2, 8, 128), F32),
            pltpu.VMEM((2, 2, 8, 128), F32),
            pltpu.VMEM((16, 8, 128), F32),
            pltpu.VMEM((8, 8, 128), F32),
            sem((2, NT)), sem((NT,)), sem((5, NT)), sem((5, 3, NT)),
            sem((2, 2, NT, NH)), sem((2, 2, NT, NH)), sem((2, 2, NT + 1, 2)), sem((2, 2, NT + 1, 2)),
            sem((2, 2)), sem((2, 2)), sem((15,)), sem((15,)), sem((7,)), sem((7,)),
        ],
        compiler_params=pltpu.CompilerParams(
            collective_id=0, has_side_effects=True, vmem_limit_bytes=24 * 1024 * 1024
        ),
    )(*[pltpu.with_memory_space_constraint(a, pltpu.HBM) for a in (right_side, reaction, velocity)])
    return sol, res, norm.reshape(())


def solution(mesh):
    spec = P("gx", "gy", "gz")
    return jax.shard_map(
        local,
        mesh=mesh,
        in_specs=(spec, spec, P(None, "gx", "gy", "gz")),
        out_specs=(spec, spec, P()),
        check_vma=False,
    )
```

```python
import functools

import jax
import jax.numpy as jnp
from jax import lax
from jax.experimental import pallas as pl
from jax.experimental.pallas import tpu as pltpu
from jax.sharding import PartitionSpec as P

ITERS = 5
centre = 7.25
half_width = 6.75
MESH = pl.DeviceIdType.MESH
F32 = jnp.float32


def chebyshev_weights(count):
    ratio_value = centre / half_width
    weights = [1.0 / ratio_value]
    for iteration in range(count):
        weights.append(1.0 / (2.0 * ratio_value - weights[-1]))
    return weights


NXL, NYL, NT = 16, 64, 4
NJ = NYL // 8
TOP = 8
NH = 2
CELLS = 256 * 256 * 1024
SLABS = ((0, 1), (15, 1), (1, 4), (5, 4), (9, 6))


def kernel(
    rhs, rea, vel, sol, res, norm,
    D0, D1, R, S, V, C, ZS, ZH, G1, G2,
    lf, lr, lc, lv, xs, xr, ys, yr, zs, zr, g1s, g1r, g2s, g2r,
):
    gx, gy, gz = lax.axis_index("gx"), lax.axis_index("gy"), lax.axis_index("gz")
    px, py = gx // 4, gx % 4
    yz = gy * 2 + gz
    weights = chebyshev_weights(ITERS)
    D = (D0, D1)

    barrier = pltpu.get_barrier_semaphore()
    near = [(gx + 1) % 16, (gx + 15) % 16]
    ring_y = [px * 4 + (py + o) % 4 for o in (1, 2, 3)]
    ring_x = [(gx + 4 * o) % 16 for o in (1, 2, 3)]
    block = [(yz + o) % 8 for o in range(1, 8)]
    peers = [(g, gy, gz) for g in near + ring_y + ring_x] + [(gx, b // 2, b % 2) for b in block]
    for peer in peers:
        pl.semaphore_signal(barrier, inc=1, device_id=peer, device_id_type=MESH)

    def rhs_load(x0, n, t, sem):
        return pltpu.make_async_copy(
            rhs.at[pl.ds(x0, n), :, pl.ds(128 * t, 128)],
            D0.at[pl.ds(x0 + 1, n), t, pl.ds(TOP, NYL), :],
            sem,
        )

    face_loads = [rhs_load(x0, 1, t, lf.at[i, t]) for t in range(NT) for i, x0 in enumerate((0, NXL - 1))]
    rest = [rhs_load(1, NXL - 2, t, lr.at[t]) for t in range(NT)]

    def coef_load(x0, n, i):
        out = []
        for t in range(NT):
            lanes = pl.ds(128 * t, 128)
            out.append(pltpu.make_async_copy(rea.at[pl.ds(x0, n), :, lanes], C.at[pl.ds(x0, n), t], lc.at[i, t]))
            out += [
                pltpu.make_async_copy(
                    vel.at[c, pl.ds(x0, n), :, lanes], V.at[c, pl.ds(x0, n), t], lv.at[i, c, t]
                )
                for c in range(3)
            ]
        return out

    slabs = [coef_load(x0, n, i) for i, (x0, n) in enumerate(SLABS)]
    for copy in face_loads + rest + sum(slabs, []):
        copy.start()

    zrow = jnp.zeros((1, 128), F32)

    def zero_rows(row):
        def body(x, carry):
            for b in range(2):
                for t in range(NT):
                    D[b][x, t, pl.ds(row, 1), :] = zrow
            return carry

        lax.fori_loop(1, NXL + 1, body, 0)

    @pl.when(gy == 0)
    def _():
        zero_rows(TOP - 1)

    @pl.when(gy == 3)
    def _():
        zero_rows(TOP + NYL)

    for copy in face_loads:
        copy.wait()
    pl.semaphore_wait(barrier, len(peers))

    x_side = (
        (1, NXL + 1, (gx + 15) % 16),
        (NXL, 0, (gx + 1) % 16),
    )

    def tile(t):
        return t + gz * (NT - 1 - 2 * t)

    def x_copy(buf, side, t, h):
        src, dst, to = x_side[side]
        rows = pl.ds(TOP + h * (NYL // NH), NYL // NH)
        return pltpu.make_async_remote_copy(
            src_ref=D[buf].at[src, tile(t), rows, :],
            dst_ref=D[buf].at[dst, tile(t), rows, :],
            send_sem=xs.at[buf, side, t, h],
            recv_sem=xr.at[buf, side, t, h],
            device_id=(to, gy, gz),
            device_id_type=MESH,
        )

    def x_each(buf, t, h, what):
        for side in range(2):
            getattr(x_copy(buf, side, t, h), what)()

    chunks = [(t, h) for t in range(NT) for h in range(NH)]

    y_side = (
        (TOP, TOP + NYL, gy - 1, gy > 0, gy < 3),
        (TOP + NYL - 1, TOP - 1, gy + 1, gy < 3, gy > 0),
    )

    def y_copies(buf, side, chunk):
        src, dst, to, _, _ = y_side[side]
        if chunk == 0:
            parts = [(pl.ds(2, NXL - 2), slice(None), 0)]
        else:
            parts = [(pl.ds(x, 1), pl.ds(tile(chunk - 1), 1), i) for i, x in enumerate((1, NXL))]
        return [
            pltpu.make_async_remote_copy(
                src_ref=D[buf].at[xs_, ts_, pl.ds(src, 1), :],
                dst_ref=D[buf].at[xs_, ts_, pl.ds(dst, 1), :],
                send_sem=ys.at[buf, side, chunk, i],
                recv_sem=yr.at[buf, side, chunk, i],
                device_id=(gx, to, gz),
                device_id_type=MESH,
            )
            for xs_, ts_, i in parts
        ]

    def y_each(buf, chunk, what, which=(0, 1)):
        def act(side):
            for copy in y_copies(buf, side, chunk):
                getattr(copy, what)()

        for side in which:
            sends, gets = y_side[side][3:]
            pl.when(gets if what == "wait_recv" else sends)(functools.partial(act, side))

    def z_copy(buf, part):
        return pltpu.make_async_remote_copy(
            src_ref=ZS.at[buf, part],
            dst_ref=ZH.at[buf, part],
            send_sem=zs.at[buf, part],
            recv_sem=zr.at[buf, part],
            device_id=(gx, gy, 1 - gz),
            device_id_type=MESH,
        )

    lane = lax.broadcasted_iota(jnp.int32, (8, 128), 1)
    first_lane, last_lane = lane == 0, lane == 127
    z_tile = (NT - 1) * (1 - gz)
    low = gz.astype(F32)
    high = 1.0 - low

    middle = range(1, NJ - 1)

    def z_pack(buf, part):
        def add(x, js, acc):
            for j in js:
                v = (x - 1) * NJ + j
                cell = D[buf][x, z_tile, pl.ds(TOP + 8 * j, 8), :]
                cell = pltpu.roll(cell, (v + 1 - gz) & 127, 1)
                acc = jnp.where(lane == v, cell, acc)
            return acc

        acc = jnp.zeros((8, 128), F32)
        if part == 0:
            acc = lax.fori_loop(0, 4, lambda i, acc: add(3 + 2 * i, range(NJ), add(2 + 2 * i, range(NJ), acc)), acc)
            for x in range(10, NXL):
                acc = add(x, (0, NJ - 1), acc)
        elif part == 1:
            acc = add(NXL, range(NJ), add(1, range(NJ), acc))
        else:
            acc = lax.fori_loop(
                0, 2, lambda i, acc: add(12 + 3 * i, middle, add(11 + 3 * i, middle, add(10 + 3 * i, middle, acc))), acc
            )
        ZS[buf, part] = acc

    def row_group(step, x, j, tiles, halo, sums=None):
        now = D[step % 2]
        row = TOP + 8 * j
        lines = pl.ds(8 * j, 8)
        cells, ups, downs, stores = {}, {}, {}, []

        def cell(t):
            if t not in cells:
                cells[t] = now[x, t, pl.ds(row, 8), :]
            return cells[t]

        def up(t):
            if t not in ups:
                ups[t] = pltpu.roll(cell(t), 127, 1)
            return ups[t]

        def down(t):
            if t not in downs:
                downs[t] = pltpu.roll(cell(t), 1, 1)
            return downs[t]

        if 0 in tiles or NT - 1 in tiles:
            v = (x - 1) * NJ + j
            beyond = pltpu.roll(halo, (127 * (1 - gz) - v) & 127, 1)
        for t in tiles:
            m = cell(t)
            zm = jnp.where(first_lane, down(t - 1) if t else beyond * low, down(t))
            zp = jnp.where(last_lane, up(t + 1) if t < NT - 1 else beyond * high, up(t))
            stores += cell_step(step, x, t, row, lines, m, zm, zp, sums, t)
        return stores

    def face_group(step, x, j, t, halo, sums=None):
        now = D[step % 2]
        row = TOP + 8 * j
        lines, rows = pl.ds(8 * j, 8), pl.ds(row, 8)
        at_t = tile(t)
        m = now[x, at_t, rows, :]
        down, up = pltpu.roll(m, 1, 1), pltpu.roll(m, 127, 1)
        before = pltpu.roll(now[x, jnp.maximum(at_t - 1, 0), rows, :], 1, 1)
        after = pltpu.roll(now[x, jnp.minimum(at_t + 1, NT - 1), rows, :], 127, 1)
        if t == 0:
            before, after = before * low, after * high
        if t == NT - 1:
            v = (x - 1) * NJ + j
            beyond = pltpu.roll(halo, (127 * (1 - gz) - v) & 127, 1)
            before = before * high + beyond * low
            after = after * low + beyond * high
        zm = jnp.where(first_lane, before, down)
        zp = jnp.where(last_lane, after, up)
        return cell_step(step, x, at_t, row, lines, m, zm, zp, sums, t)

    def cell_step(step, x, t, row, lines, m, zm, zp, sums, slot):
        now, new = D[step % 2], D[(step + 1) % 2]
        xm = now[x - 1, t, pl.ds(row, 8), :]
        xp = now[x + 1, t, pl.ds(row, 8), :]
        ym = now[x, t, pl.ds(row - 1, 8), :]
        yp = now[x, t, pl.ds(row + 1, 8), :]
        at = (x - 1, t, lines, slice(None))
        vx, vy, vz = (V[(c,) + at] for c in range(3))
        flow = vx * (xp - xm) + vy * (yp - ym) + vz * (zp - zm)
        beside = ((xp + xm) + (yp + ym)) + (zp + zm)
        applied = (6.0 + C[at]) * m - (beside - flow)
        lanes = pl.ds(128 * t if isinstance(t, int) else pl.multiple_of(128 * t, 128), 128)
        out = (x - 1, lines, lanes)
        if step == 0:
            r = m - applied * (1.0 / centre)
            alpha = weights[1] * weights[0] / centre
        else:
            r = R[at] - applied
            alpha = weights[step + 1] * weights[step] if step + 1 < ITERS else 0.0
        if step + 1 == ITERS:
            sums[slot] = sums[slot] + r * r
            return [(res, out, r)]
        d = alpha * m + (2.0 * weights[step + 1] / half_width) * r
        s = (m * (1.0 / centre) if step == 0 else S[at]) + d
        return [
            (R, at, r),
            (new, (x, t, pl.ds(row, 8), slice(None)), d),
            (S, at, s) if step + 2 < ITERS else (sol, out, s),
        ]

    def late(parts):
        held = []
        for part in parts:
            stores = part()
            for ref, at, value in held:
                ref[at] = value
            held = stores
        for ref, at, value in held:
            ref[at] = value

    def groups(step, items, halo, sums=None):
        late([functools.partial(row_group, step, x, j, range(NT), halo, sums) for x, j in items])

    def layers(step, first, count, js, halo, many, sums):
        def body(i, carry):
            part = list(carry)
            groups(step, [(first + i * many + k, j) for k in range(many) for j in js], halo, part)
            return tuple(part)

        sums[:] = lax.fori_loop(0, count // many, body, tuple(sums))

    def faces(step, t, h, sums=None):
        js = range(h * (NJ // NH), (h + 1) * (NJ // NH))
        halo = ZH[step % 2, 1]
        late([functools.partial(face_group, step, x, j, t, halo, sums) for j in js for x in (1, NXL)])

    for t, h in chunks:
        x_each(0, t, h, "start")
    for copy in rest:
        copy.wait()
    for chunk in range(NT + 1):
        y_each(0, chunk, "start")
    for part in range(3):
        z_pack(0, part)
        z_copy(0, part).start()

    for step in range(ITERS):
        cur, new, more = step % 2, (step + 1) % 2, step + 1 < ITERS
        y_each(cur, 0, "wait_recv")
        z_copy(cur, 0).wait_recv()
        halo = ZH[cur, 0]
        sums = [] if more else [jnp.zeros((8, 128), F32)] * NT
        if step == 0:
            for copy in slabs[0] + slabs[1] + slabs[2]:
                copy.wait()
            layers(step, 2, 4, range(NJ), halo, 2, sums)
            for copy in slabs[3]:
                copy.wait()
            layers(step, 6, 4, range(NJ), halo, 2, sums)
            for copy in slabs[4]:
                copy.wait()
            layers(step, 10, 6, (0, NJ - 1), halo, 6, sums)
            y_each(new, 0, "start")
        else:
            layers(step, 2, NXL - 2, (0, NJ - 1), halo, 7, sums)
            if more:
                y_each(new, 0, "start")
            layers(step, 2, 8, middle, halo, 2, sums)
        if more:
            z_pack(new, 0)
            z_copy(new, 0).start()
        for t, h in chunks:
            x_each(cur, t, h, "wait_recv")
            if h == 0:
                y_each(cur, t + 1, "wait_recv", (1,))
            if h == NH - 1:
                y_each(cur, t + 1, "wait_recv", (0,))
            if (t, h) == (NT - 1, 0):
                z_copy(cur, 1).wait_recv()
            faces(step, t, h, sums)
            if more:
                x_each(new, t, h, "start")
                if h == 0:
                    y_each(new, t + 1, "start", (0,))
                if h == NH - 1:
                    y_each(new, t + 1, "start", (1,))
            place = t * NH + h
            if place == 0:
                z_copy(cur, 2).wait_recv()
            if place < 3:
                groups(step, [(10 + 2 * place + k, j) for k in range(2) for j in middle], ZH[cur, 2], sums)
            if place == 3 and more:
                z_pack(new, 2)
                z_copy(new, 2).start()
        if more:
            z_pack(new, 1)
            z_copy(new, 1).start()
            for t, h in chunks:
                x_each(cur, t, h, "wait_send")
            for chunk in range(NT + 1):
                y_each(cur, chunk, "wait_send")
            for part in range(3):
                z_copy(cur, part).wait_send()
    total = jnp.sum((sums[0] + sums[1]) + (sums[2] + sums[3]), axis=0, keepdims=True)

    def stage(total, G, send, recv, own, count, place):
        G[own, pl.ds(0, 1), :] = total
        copies = [
            pltpu.make_async_remote_copy(
                src_ref=G.at[own, pl.ds(0, 1), :],
                dst_ref=G.at[own, pl.ds(0, 1), :],
                send_sem=send.at[o - 1],
                recv_sem=recv.at[o - 1],
                device_id=place((own + o) % count),
                device_id_type=MESH,
            )
            for o in range(1, count)
        ]
        for copy in copies:
            copy.start()
        for copy in copies:
            copy.wait_recv()
        parts = [G[i, pl.ds(0, 1), :] for i in range(count)]
        while len(parts) > 1:
            parts = [a + b for a, b in zip(parts[::2], parts[1::2])]
        return parts[0], copies

    total, c1 = stage(total, G1, g1s, g1r, gx, 16, lambda p: (p, gy, gz))
    total, c2 = stage(total, G2, g2s, g2r, yz, 8, lambda p: (gx, p // 2, p % 2))
    whole = jnp.sum(total, axis=1, keepdims=True)
    norm[...] = jnp.sqrt(whole * (1.0 / CELLS) + 1e-06)
    cur = (ITERS - 1) % 2
    for t, h in chunks:
        x_each(cur, t, h, "wait_send")
    for chunk in range(NT + 1):
        y_each(cur, chunk, "wait_send")
    for part in range(3):
        z_copy(cur, part).wait_send()
    for copy in c1 + c2:
        copy.wait_send()


def local(right_side, reaction, velocity):
    sem = pltpu.SemaphoreType.DMA
    shape = right_side.shape
    sol, res, norm = pl.pallas_call(
        kernel,
        name="chebyshev",
        out_shape=(pltpu.VMEM(shape, F32), pltpu.VMEM(shape, F32), jax.ShapeDtypeStruct((1, 1), F32)),
        in_specs=[pl.BlockSpec(memory_space=pltpu.HBM)] * 3,
        out_specs=(pl.BlockSpec(memory_space=pltpu.VMEM),) * 3,
        scratch_shapes=[
            pltpu.VMEM((NXL + 2, NT, NYL + 16, 128), F32),
            pltpu.VMEM((NXL + 2, NT, NYL + 16, 128), F32),
            pltpu.VMEM((NXL, NT, NYL, 128), F32),
            pltpu.VMEM((NXL, NT, NYL, 128), F32),
            pltpu.VMEM((3, NXL, NT, NYL, 128), F32),
            pltpu.VMEM((NXL, NT, NYL, 128), F32),
            pltpu.VMEM((2, 3, 8, 128), F32),
            pltpu.VMEM((2, 3, 8, 128), F32),
            pltpu.VMEM((16, 8, 128), F32),
            pltpu.VMEM((8, 8, 128), F32),
            sem((2, NT)), sem((NT,)), sem((5, NT)), sem((5, 3, NT)),
            sem((2, 2, NT, NH)), sem((2, 2, NT, NH)), sem((2, 2, NT + 1, 2)), sem((2, 2, NT + 1, 2)),
            sem((2, 3)), sem((2, 3)), sem((15,)), sem((15,)), sem((7,)), sem((7,)),
        ],
        compiler_params=pltpu.CompilerParams(
            collective_id=0, has_side_effects=True, vmem_limit_bytes=24 * 1024 * 1024
        ),
    )(*[pltpu.with_memory_space_constraint(a, pltpu.HBM) for a in (right_side, reaction, velocity)])
    return sol, res, norm.reshape(())


def solution(mesh):
    spec = P("gx", "gy", "gz")
    return jax.shard_map(
        local,
        mesh=mesh,
        in_specs=(spec, spec, P(None, "gx", "gy", "gz")),
        out_specs=(spec, spec, P()),
        check_vma=False,
    )
```

```python
import functools

import jax
import jax.numpy as jnp
from jax import lax
from jax.experimental import pallas as pl
from jax.experimental.pallas import tpu as pltpu
from jax.sharding import PartitionSpec as P

ITERS = 5
centre = 7.25
half_width = 6.75
MESH = pl.DeviceIdType.MESH
F32 = jnp.float32


def chebyshev_weights(count):
    ratio_value = centre / half_width
    weights = [1.0 / ratio_value]
    for iteration in range(count):
        weights.append(1.0 / (2.0 * ratio_value - weights[-1]))
    return weights


NXL, NYL, NT = 16, 64, 4
NJ = NYL // 8
TOP = 8
NH = 4
CELLS = 256 * 256 * 1024
SLABS = ((0, 1), (15, 1), (1, 4), (5, 4), (9, 6))


def kernel(
    rhs, rea, vel, sol, res, norm,
    D0, D1, R, S, V, C, ZS, ZH, G1, G2,
    lf, lr, lc, lv, xs, xr, ys, yr, zs, zr, g1s, g1r, g2s, g2r,
):
    gx, gy, gz = lax.axis_index("gx"), lax.axis_index("gy"), lax.axis_index("gz")
    px, py = gx // 4, gx % 4
    yz = gy * 2 + gz
    weights = chebyshev_weights(ITERS)
    D = (D0, D1)

    barrier = pltpu.get_barrier_semaphore()
    near = [(gx + 1) % 16, (gx + 15) % 16]
    ring_y = [px * 4 + (py + o) % 4 for o in (1, 2, 3)]
    ring_x = [(gx + 4 * o) % 16 for o in (1, 2, 3)]
    block = [(yz + o) % 8 for o in range(1, 8)]
    peers = [(g, gy, gz) for g in near + ring_y + ring_x] + [(gx, b // 2, b % 2) for b in block]
    for peer in peers:
        pl.semaphore_signal(barrier, inc=1, device_id=peer, device_id_type=MESH)

    def rhs_load(x0, n, t, sem):
        return pltpu.make_async_copy(
            rhs.at[pl.ds(x0, n), :, pl.ds(128 * t, 128)],
            D0.at[pl.ds(x0 + 1, n), t, pl.ds(TOP, NYL), :],
            sem,
        )

    face_loads = [rhs_load(x0, 1, t, lf.at[i, t]) for t in range(NT) for i, x0 in enumerate((0, NXL - 1))]
    rest = [rhs_load(1, NXL - 2, t, lr.at[t]) for t in range(NT)]

    def coef_load(x0, n, i):
        out = []
        for t in range(NT):
            lanes = pl.ds(128 * t, 128)
            out.append(pltpu.make_async_copy(rea.at[pl.ds(x0, n), :, lanes], C.at[pl.ds(x0, n), t], lc.at[i, t]))
            out += [
                pltpu.make_async_copy(
                    vel.at[c, pl.ds(x0, n), :, lanes], V.at[c, pl.ds(x0, n), t], lv.at[i, c, t]
                )
                for c in range(3)
            ]
        return out

    slabs = [coef_load(x0, n, i) for i, (x0, n) in enumerate(SLABS)]
    for copy in face_loads + rest + sum(slabs, []):
        copy.start()

    zrow = jnp.zeros((1, 128), F32)

    def zero_rows(row):
        def body(x, carry):
            for b in range(2):
                for t in range(NT):
                    D[b][x, t, pl.ds(row, 1), :] = zrow
            return carry

        lax.fori_loop(1, NXL + 1, body, 0)

    @pl.when(gy == 0)
    def _():
        zero_rows(TOP - 1)

    @pl.when(gy == 3)
    def _():
        zero_rows(TOP + NYL)

    for copy in face_loads:
        copy.wait()
    pl.semaphore_wait(barrier, len(peers))

    x_side = (
        (1, NXL + 1, (gx + 15) % 16),
        (NXL, 0, (gx + 1) % 16),
    )

    def tile(t):
        return t + gz * (NT - 1 - 2 * t)

    def x_copy(buf, side, t, h):
        src, dst, to = x_side[side]
        rows = pl.ds(TOP + h * (NYL // NH), NYL // NH)
        return pltpu.make_async_remote_copy(
            src_ref=D[buf].at[src, tile(t), rows, :],
            dst_ref=D[buf].at[dst, tile(t), rows, :],
            send_sem=xs.at[buf, side, t, h],
            recv_sem=xr.at[buf, side, t, h],
            device_id=(to, gy, gz),
            device_id_type=MESH,
        )

    def x_each(buf, t, h, what):
        for side in range(2):
            getattr(x_copy(buf, side, t, h), what)()

    chunks = [(t, h) for t in range(NT) for h in range(NH)]

    y_side = (
        (TOP, TOP + NYL, gy - 1, gy > 0, gy < 3),
        (TOP + NYL - 1, TOP - 1, gy + 1, gy < 3, gy > 0),
    )

    def y_copies(buf, side, chunk):
        src, dst, to, _, _ = y_side[side]
        if isinstance(chunk, int) and chunk == 0:
            parts = [(pl.ds(2, NXL - 2), slice(None), 0)]
        else:
            parts = [(pl.ds(x, 1), pl.ds(tile(chunk - 1), 1), i) for i, x in enumerate((1, NXL))]
        return [
            pltpu.make_async_remote_copy(
                src_ref=D[buf].at[xs_, ts_, pl.ds(src, 1), :],
                dst_ref=D[buf].at[xs_, ts_, pl.ds(dst, 1), :],
                send_sem=ys.at[buf, side, chunk, i],
                recv_sem=yr.at[buf, side, chunk, i],
                device_id=(gx, to, gz),
                device_id_type=MESH,
            )
            for xs_, ts_, i in parts
        ]

    def y_each(buf, chunk, what, which=(0, 1)):
        def act(side):
            for copy in y_copies(buf, side, chunk):
                getattr(copy, what)()

        for side in which:
            sends, gets = y_side[side][3:]
            pl.when(gets if what == "wait_recv" else sends)(functools.partial(act, side))

    def z_copy(buf, part):
        return pltpu.make_async_remote_copy(
            src_ref=ZS.at[buf, part],
            dst_ref=ZH.at[buf, part],
            send_sem=zs.at[buf, part],
            recv_sem=zr.at[buf, part],
            device_id=(gx, gy, 1 - gz),
            device_id_type=MESH,
        )

    lane = lax.broadcasted_iota(jnp.int32, (8, 128), 1)
    first_lane, last_lane = lane == 0, lane == 127
    z_tile = (NT - 1) * (1 - gz)
    low = gz.astype(F32)
    high = 1.0 - low

    middle = range(1, NJ - 1)

    def z_pack(buf, part):
        def add(x, js, acc):
            for j in js:
                v = (x - 1) * NJ + j
                cell = D[buf][x, z_tile, pl.ds(TOP + 8 * j, 8), :]
                cell = pltpu.roll(cell, (v + 1 - gz) & 127, 1)
                acc = jnp.where(lane == v, cell, acc)
            return acc

        acc = jnp.zeros((8, 128), F32)
        if part == 0:
            acc = lax.fori_loop(0, 4, lambda i, acc: add(3 + 2 * i, range(NJ), add(2 + 2 * i, range(NJ), acc)), acc)
            for x in range(10, NXL):
                acc = add(x, (0, NJ - 1), acc)
        elif part == 1:
            acc = add(NXL, range(NJ), add(1, range(NJ), acc))
        else:
            acc = lax.fori_loop(
                0, 2, lambda i, acc: add(12 + 3 * i, middle, add(11 + 3 * i, middle, add(10 + 3 * i, middle, acc))), acc
            )
        ZS[buf, part] = acc

    def row_group(step, x, j, tiles, halo, sums=None):
        now = D[step % 2]
        row = TOP + 8 * j
        lines = pl.ds(8 * j, 8)
        cells, ups, downs, stores = {}, {}, {}, []

        def cell(t):
            if t not in cells:
                cells[t] = now[x, t, pl.ds(row, 8), :]
            return cells[t]

        def up(t):
            if t not in ups:
                ups[t] = pltpu.roll(cell(t), 127, 1)
            return ups[t]

        def down(t):
            if t not in downs:
                downs[t] = pltpu.roll(cell(t), 1, 1)
            return downs[t]

        if 0 in tiles or NT - 1 in tiles:
            v = (x - 1) * NJ + j
            beyond = pltpu.roll(halo, (127 * (1 - gz) - v) & 127, 1)
        for t in tiles:
            m = cell(t)
            zm = jnp.where(first_lane, down(t - 1) if t else beyond * low, down(t))
            zp = jnp.where(last_lane, up(t + 1) if t < NT - 1 else beyond * high, up(t))
            stores += cell_step(step, x, t, row, lines, m, zm, zp, sums, t)
        return stores

    def face_group(step, x, j, t, halo, sums=None):
        now = D[step % 2]
        row = TOP + 8 * j
        lines, rows = pl.ds(8 * j, 8), pl.ds(row, 8)
        at_t = tile(t)
        m = now[x, at_t, rows, :]
        down, up = pltpu.roll(m, 1, 1), pltpu.roll(m, 127, 1)
        before = pltpu.roll(now[x, jnp.maximum(at_t - 1, 0), rows, :], 1, 1)
        after = pltpu.roll(now[x, jnp.minimum(at_t + 1, NT - 1), rows, :], 127, 1)
        if isinstance(t, int):
            v = (x - 1) * NJ + j
            beyond = pltpu.roll(halo, (127 * (1 - gz) - v) & 127, 1)
            before = before * high + beyond * low
            after = after * low + beyond * high
        else:
            outer = jnp.where(t == 0, 1.0, 0.0)
            before, after = before * (1.0 - outer * high), after * (1.0 - outer * low)
        zm = jnp.where(first_lane, before, down)
        zp = jnp.where(last_lane, after, up)
        return cell_step(step, x, at_t, row, lines, m, zm, zp, sums, j % NT)

    def cell_step(step, x, t, row, lines, m, zm, zp, sums, slot):
        now, new = D[step % 2], D[(step + 1) % 2]
        xm = now[x - 1, t, pl.ds(row, 8), :]
        xp = now[x + 1, t, pl.ds(row, 8), :]
        ym = now[x, t, pl.ds(row - 1, 8), :]
        yp = now[x, t, pl.ds(row + 1, 8), :]
        at = (x - 1, t, lines, slice(None))
        vx, vy, vz = (V[(c,) + at] for c in range(3))
        flow = vx * (xp - xm) + vy * (yp - ym) + vz * (zp - zm)
        beside = ((xp + xm) + (yp + ym)) + (zp + zm)
        applied = (6.0 + C[at]) * m - (beside - flow)
        lanes = pl.ds(128 * t if isinstance(t, int) else pl.multiple_of(128 * t, 128), 128)
        out = (x - 1, lines, lanes)
        if step == 0:
            r = m - applied * (1.0 / centre)
            alpha = weights[1] * weights[0] / centre
        else:
            r = R[at] - applied
            alpha = weights[step + 1] * weights[step] if step + 1 < ITERS else 0.0
        if step + 1 == ITERS:
            sums[slot] = sums[slot] + r * r
            return [(res, out, r)]
        d = alpha * m + (2.0 * weights[step + 1] / half_width) * r
        s = (m * (1.0 / centre) if step == 0 else S[at]) + d
        return [
            (R, at, r),
            (new, (x, t, pl.ds(row, 8), slice(None)), d),
            (S, at, s) if step + 2 < ITERS else (sol, out, s),
        ]

    def late(parts):
        held = []
        for part in parts:
            stores = part()
            for ref, at, value in held:
                ref[at] = value
            held = stores
        for ref, at, value in held:
            ref[at] = value

    def groups(step, items, halo, sums=None):
        late([functools.partial(row_group, step, x, j, range(NT), halo, sums) for x, j in items])

    def layers(step, first, count, js, halo, many, sums):
        def body(i, carry):
            part = list(carry)
            groups(step, [(first + i * many + k, j) for k in range(many) for j in js], halo, part)
            return tuple(part)

        sums[:] = lax.fori_loop(0, count // many, body, tuple(sums))

    def faces(step, t, sums):
        cur, new, more = step % 2, (step + 1) % 2, step + 1 < ITERS
        for h in range(NH):
            x_each(cur, t, h, "wait_recv")
            if h == 0:
                y_each(cur, t + 1, "wait_recv", (1,))
            if h == NH - 1:
                y_each(cur, t + 1, "wait_recv", (0,))
            js = range(h * (NJ // NH), (h + 1) * (NJ // NH))
            halo = ZH[cur, 1] if isinstance(t, int) else None
            late([functools.partial(face_group, step, x, j, t, halo, sums) for j in js for x in (1, NXL)])
            if more:
                x_each(new, t, h, "start")
                if h == 0:
                    y_each(new, t + 1, "start", (0,))
                if h == NH - 1:
                    y_each(new, t + 1, "start", (1,))

    for t, h in chunks:
        x_each(0, t, h, "start")
    for copy in rest:
        copy.wait()
    for chunk in range(NT + 1):
        y_each(0, chunk, "start")
    for part in range(3):
        z_pack(0, part)
        z_copy(0, part).start()

    for step in range(ITERS):
        cur, new, more = step % 2, (step + 1) % 2, step + 1 < ITERS
        y_each(cur, 0, "wait_recv")
        z_copy(cur, 0).wait_recv()
        halo = ZH[cur, 0]
        sums = [] if more else [jnp.zeros((8, 128), F32)] * NT
        if step == 0:
            for copy in slabs[0] + slabs[1] + slabs[2]:
                copy.wait()
            layers(step, 2, 4, range(NJ), halo, 2, sums)
            for copy in slabs[3]:
                copy.wait()
            layers(step, 6, 4, range(NJ), halo, 2, sums)
            for copy in slabs[4]:
                copy.wait()
            layers(step, 10, 6, (0, NJ - 1), halo, 6, sums)
            y_each(new, 0, "start")
        else:
            layers(step, 2, NXL - 2, (0, NJ - 1), halo, 7, sums)
            if more:
                y_each(new, 0, "start")
            layers(step, 2, 8, middle, halo, 2, sums)
        if more:
            z_pack(new, 0)
            z_copy(new, 0).start()
        def face_tile(t, carry):
            part = list(carry)
            faces(step, t, part)
            pl.when(t == 0)(lambda: z_copy(cur, 2).wait_recv())
            groups(step, [(10 + 2 * t + k, j) for k in range(2) for j in middle], ZH[cur, 2], part)
            return tuple(part)

        sums = list(lax.fori_loop(0, NT - 1, face_tile, tuple(sums)))
        if more:
            z_pack(new, 2)
            z_copy(new, 2).start()
        z_copy(cur, 1).wait_recv()
        faces(step, NT - 1, sums)
        if more:
            z_pack(new, 1)
            z_copy(new, 1).start()
            for t, h in chunks:
                x_each(cur, t, h, "wait_send")
            for chunk in range(NT + 1):
                y_each(cur, chunk, "wait_send")
            for part in range(3):
                z_copy(cur, part).wait_send()
    total = jnp.sum((sums[0] + sums[1]) + (sums[2] + sums[3]), axis=0, keepdims=True)

    def stage(total, G, send, recv, own, count, place, order, meanwhile):
        G[own, pl.ds(0, 1), :] = total
        copies = [
            pltpu.make_async_remote_copy(
                src_ref=G.at[own, pl.ds(0, 1), :],
                dst_ref=G.at[own, pl.ds(0, 1), :],
                send_sem=send.at[o - 1],
                recv_sem=recv.at[o - 1],
                device_id=place((own + o) % count),
                device_id_type=MESH,
            )
            for o in order
        ]
        for copy in copies:
            copy.start()
        meanwhile()
        for copy in copies:
            copy.wait_recv()
        parts = [G[i, pl.ds(0, 1), :] for i in range(count)]
        while len(parts) > 1:
            parts = [a + b for a, b in zip(parts[::2], parts[1::2])]
        return parts[0], copies

    def last_sends():
        cur = (ITERS - 1) % 2
        for t, h in chunks:
            x_each(cur, t, h, "wait_send")
        for chunk in range(NT + 1):
            y_each(cur, chunk, "wait_send")
        for part in range(3):
            z_copy(cur, part).wait_send()

    far_first = (10, 6, 9, 11, 7, 5, 2, 14, 8, 3, 13, 1, 15, 4, 12)
    total, c1 = stage(total, G1, g1s, g1r, gx, 16, lambda p: (p, gy, gz), far_first, last_sends)
    total, c2 = stage(total, G2, g2s, g2r, yz, 8, lambda p: (gx, p // 2, p % 2), range(1, 8), lambda: None)
    whole = jnp.sum(total, axis=1, keepdims=True)
    norm[...] = jnp.sqrt(whole * (1.0 / CELLS) + 1e-06)
    for copy in c1 + c2:
        copy.wait_send()


def local(right_side, reaction, velocity):
    sem = pltpu.SemaphoreType.DMA
    shape = right_side.shape
    sol, res, norm = pl.pallas_call(
        kernel,
        name="chebyshev",
        out_shape=(pltpu.VMEM(shape, F32), pltpu.VMEM(shape, F32), jax.ShapeDtypeStruct((1, 1), F32)),
        in_specs=[pl.BlockSpec(memory_space=pltpu.HBM)] * 3,
        out_specs=(pl.BlockSpec(memory_space=pltpu.VMEM),) * 3,
        scratch_shapes=[
            pltpu.VMEM((NXL + 2, NT, NYL + 16, 128), F32),
            pltpu.VMEM((NXL + 2, NT, NYL + 16, 128), F32),
            pltpu.VMEM((NXL, NT, NYL, 128), F32),
            pltpu.VMEM((NXL, NT, NYL, 128), F32),
            pltpu.VMEM((3, NXL, NT, NYL, 128), F32),
            pltpu.VMEM((NXL, NT, NYL, 128), F32),
            pltpu.VMEM((2, 3, 8, 128), F32),
            pltpu.VMEM((2, 3, 8, 128), F32),
            pltpu.VMEM((16, 8, 128), F32),
            pltpu.VMEM((8, 8, 128), F32),
            sem((2, NT)), sem((NT,)), sem((5, NT)), sem((5, 3, NT)),
            sem((2, 2, NT, NH)), sem((2, 2, NT, NH)), sem((2, 2, NT + 1, 2)), sem((2, 2, NT + 1, 2)),
            sem((2, 3)), sem((2, 3)), sem((15,)), sem((15,)), sem((7,)), sem((7,)),
        ],
        compiler_params=pltpu.CompilerParams(
            collective_id=0, has_side_effects=True, vmem_limit_bytes=24 * 1024 * 1024
        ),
    )(*[pltpu.with_memory_space_constraint(a, pltpu.HBM) for a in (right_side, reaction, velocity)])
    return sol, res, norm.reshape(())


def solution(mesh):
    spec = P("gx", "gy", "gz")
    return jax.shard_map(
        local,
        mesh=mesh,
        in_specs=(spec, spec, P(None, "gx", "gy", "gz")),
        out_specs=(spec, spec, P()),
        check_vma=False,
    )
```

```python
import functools

import jax
import jax.numpy as jnp
from jax import lax
from jax.experimental import pallas as pl
from jax.experimental.pallas import tpu as pltpu
from jax.sharding import PartitionSpec as P

ITERS = 5
centre = 7.25
half_width = 6.75
MESH = pl.DeviceIdType.MESH
F32 = jnp.float32


def chebyshev_weights(count):
    ratio_value = centre / half_width
    weights = [1.0 / ratio_value]
    for iteration in range(count):
        weights.append(1.0 / (2.0 * ratio_value - weights[-1]))
    return weights


NXL, NYL, NT = 16, 64, 4
NJ = NYL // 8
TOP = 8
NH = 2
CELLS = 256 * 256 * 1024
SLABS = ((0, 1), (15, 1), (1, 4), (5, 4), (9, 6))


def kernel(
    rhs, rea, vel, sol, res, norm,
    D0, D1, R, S, V, C, ZS, ZH, G1, G2,
    lf, lr, lc, lv, xs, xr, ys, yr, zs, zr, g1s, g1r, g2s, g2r,
):
    gx, gy, gz = lax.axis_index("gx"), lax.axis_index("gy"), lax.axis_index("gz")
    px, py = gx // 4, gx % 4
    yz = gy * 2 + gz
    weights = chebyshev_weights(ITERS)
    D = (D0, D1)

    barrier = pltpu.get_barrier_semaphore()
    near = [(gx + 1) % 16, (gx + 15) % 16]
    ring_y = [px * 4 + (py + o) % 4 for o in (1, 2, 3)]
    ring_x = [(gx + 4 * o) % 16 for o in (1, 2, 3)]
    block = [(yz + o) % 8 for o in range(1, 8)]
    peers = [(g, gy, gz) for g in near + ring_y + ring_x] + [(gx, b // 2, b % 2) for b in block]
    for peer in peers:
        pl.semaphore_signal(barrier, inc=1, device_id=peer, device_id_type=MESH)

    def rhs_load(x0, n, t, sem):
        return pltpu.make_async_copy(
            rhs.at[pl.ds(x0, n), :, pl.ds(128 * t, 128)],
            D0.at[pl.ds(x0 + 1, n), t, pl.ds(TOP, NYL), :],
            sem,
        )

    face_loads = [rhs_load(x0, 1, t, lf.at[i, t]) for t in range(NT) for i, x0 in enumerate((0, NXL - 1))]
    rest = [rhs_load(1, NXL - 2, t, lr.at[t]) for t in range(NT)]

    def coef_load(x0, n, i):
        out = []
        for t in range(NT):
            lanes = pl.ds(128 * t, 128)
            out.append(pltpu.make_async_copy(rea.at[pl.ds(x0, n), :, lanes], C.at[pl.ds(x0, n), t], lc.at[i, t]))
            out += [
                pltpu.make_async_copy(
                    vel.at[c, pl.ds(x0, n), :, lanes], V.at[c, pl.ds(x0, n), t], lv.at[i, c, t]
                )
                for c in range(3)
            ]
        return out

    slabs = [coef_load(x0, n, i) for i, (x0, n) in enumerate(SLABS)]
    for copy in face_loads + rest + sum(slabs, []):
        copy.start()

    zrow = jnp.zeros((1, 128), F32)

    def zero_rows(row):
        def body(x, carry):
            for b in range(2):
                for t in range(NT):
                    D[b][x, t, pl.ds(row, 1), :] = zrow
            return carry

        lax.fori_loop(1, NXL + 1, body, 0)

    @pl.when(gy == 0)
    def _():
        zero_rows(TOP - 1)

    @pl.when(gy == 3)
    def _():
        zero_rows(TOP + NYL)

    for copy in face_loads:
        copy.wait()
    pl.semaphore_wait(barrier, len(peers))

    x_side = (
        (1, NXL + 1, (gx + 15) % 16),
        (NXL, 0, (gx + 1) % 16),
    )

    def tile(t):
        return t + gz * (NT - 1 - 2 * t)

    def x_copy(buf, side, t, h):
        src, dst, to = x_side[side]
        rows = pl.ds(TOP + h * (NYL // NH), NYL // NH)
        return pltpu.make_async_remote_copy(
            src_ref=D[buf].at[src, tile(t), rows, :],
            dst_ref=D[buf].at[dst, tile(t), rows, :],
            send_sem=xs.at[buf, side, t, h],
            recv_sem=xr.at[buf, side, t, h],
            device_id=(to, gy, gz),
            device_id_type=MESH,
        )

    def x_each(buf, t, h, what):
        for side in range(2):
            getattr(x_copy(buf, side, t, h), what)()

    chunks = [(t, h) for t in range(NT) for h in range(NH)]

    y_side = (
        (TOP, TOP + NYL, gy - 1, gy > 0, gy < 3),
        (TOP + NYL - 1, TOP - 1, gy + 1, gy < 3, gy > 0),
    )

    def y_copies(buf, side, chunk):
        src, dst, to, _, _ = y_side[side]
        if isinstance(chunk, int) and chunk == 0:
            parts = [(pl.ds(2, NXL - 2), slice(None), 0)]
        else:
            parts = [(pl.ds(x, 1), pl.ds(tile(chunk - 1), 1), i) for i, x in enumerate((1, NXL))]
        return [
            pltpu.make_async_remote_copy(
                src_ref=D[buf].at[xs_, ts_, pl.ds(src, 1), :],
                dst_ref=D[buf].at[xs_, ts_, pl.ds(dst, 1), :],
                send_sem=ys.at[buf, side, chunk, i],
                recv_sem=yr.at[buf, side, chunk, i],
                device_id=(gx, to, gz),
                device_id_type=MESH,
            )
            for xs_, ts_, i in parts
        ]

    def y_each(buf, chunk, what, which=(0, 1)):
        def act(side):
            for copy in y_copies(buf, side, chunk):
                getattr(copy, what)()

        for side in which:
            sends, gets = y_side[side][3:]
            pl.when(gets if what == "wait_recv" else sends)(functools.partial(act, side))

    def z_copy(buf, part):
        return pltpu.make_async_remote_copy(
            src_ref=ZS.at[buf, part],
            dst_ref=ZH.at[buf, part],
            send_sem=zs.at[buf, part],
            recv_sem=zr.at[buf, part],
            device_id=(gx, gy, 1 - gz),
            device_id_type=MESH,
        )

    lane = lax.broadcasted_iota(jnp.int32, (8, 128), 1)
    first_lane, last_lane = lane == 0, lane == 127
    z_tile = (NT - 1) * (1 - gz)
    low = gz.astype(F32)
    high = 1.0 - low

    middle = range(1, NJ - 1)

    def z_pack(buf, part):
        def add(x, js, acc):
            for j in js:
                v = (x - 1) * NJ + j
                cell = D[buf][x, z_tile, pl.ds(TOP + 8 * j, 8), :]
                cell = pltpu.roll(cell, (v + 1 - gz) & 127, 1)
                acc = jnp.where(lane == v, cell, acc)
            return acc

        acc = jnp.zeros((8, 128), F32)
        if part == 0:
            acc = lax.fori_loop(0, 4, lambda i, acc: add(3 + 2 * i, range(NJ), add(2 + 2 * i, range(NJ), acc)), acc)
            for x in range(10, NXL):
                acc = add(x, (0, NJ - 1), acc)
        elif part == 1:
            acc = add(NXL, range(NJ), add(1, range(NJ), acc))
        else:
            acc = lax.fori_loop(
                0, 2, lambda i, acc: add(12 + 3 * i, middle, add(11 + 3 * i, middle, add(10 + 3 * i, middle, acc))), acc
            )
        ZS[buf, part] = acc

    def row_group(step, x, j, tiles, halo, sums=None):
        now = D[step % 2]
        row = TOP + 8 * j
        lines = pl.ds(8 * j, 8)
        cells, ups, downs, stores = {}, {}, {}, []

        def cell(t):
            if t not in cells:
                cells[t] = now[x, t, pl.ds(row, 8), :]
            return cells[t]

        def up(t):
            if t not in ups:
                ups[t] = pltpu.roll(cell(t), 127, 1)
            return ups[t]

        def down(t):
            if t not in downs:
                downs[t] = pltpu.roll(cell(t), 1, 1)
            return downs[t]

        if 0 in tiles or NT - 1 in tiles:
            v = (x - 1) * NJ + j
            beyond = pltpu.roll(halo, (127 * (1 - gz) - v) & 127, 1)
        for t in tiles:
            m = cell(t)
            zm = jnp.where(first_lane, down(t - 1) if t else beyond * low, down(t))
            zp = jnp.where(last_lane, up(t + 1) if t < NT - 1 else beyond * high, up(t))
            stores += cell_step(step, x, t, row, lines, m, zm, zp, sums, t)
        return stores

    def face_group(step, x, j, t, halo, sums=None):
        now = D[step % 2]
        row = TOP + 8 * j
        lines, rows = pl.ds(8 * j, 8), pl.ds(row, 8)
        at_t = tile(t)
        m = now[x, at_t, rows, :]
        down, up = pltpu.roll(m, 1, 1), pltpu.roll(m, 127, 1)
        before = pltpu.roll(now[x, jnp.maximum(at_t - 1, 0), rows, :], 1, 1)
        after = pltpu.roll(now[x, jnp.minimum(at_t + 1, NT - 1), rows, :], 127, 1)
        if isinstance(t, int):
            v = (x - 1) * NJ + j
            beyond = pltpu.roll(halo, (127 * (1 - gz) - v) & 127, 1)
            before = before * high + beyond * low
            after = after * low + beyond * high
        else:
            outer = jnp.where(t == 0, 1.0, 0.0)
            before, after = before * (1.0 - outer * high), after * (1.0 - outer * low)
        zm = jnp.where(first_lane, before, down)
        zp = jnp.where(last_lane, after, up)
        return cell_step(step, x, at_t, row, lines, m, zm, zp, sums, j % NT)

    def cell_step(step, x, t, row, lines, m, zm, zp, sums, slot):
        now, new = D[step % 2], D[(step + 1) % 2]
        xm = now[x - 1, t, pl.ds(row, 8), :]
        xp = now[x + 1, t, pl.ds(row, 8), :]
        ym = now[x, t, pl.ds(row - 1, 8), :]
        yp = now[x, t, pl.ds(row + 1, 8), :]
        at = (x - 1, t, lines, slice(None))
        vx, vy, vz = (V[(c,) + at] for c in range(3))
        flow = vx * (xp - xm) + vy * (yp - ym) + vz * (zp - zm)
        beside = ((xp + xm) + (yp + ym)) + (zp + zm)
        applied = (6.0 + C[at]) * m - (beside - flow)
        lanes = pl.ds(128 * t if isinstance(t, int) else pl.multiple_of(128 * t, 128), 128)
        out = (x - 1, lines, lanes)
        if step == 0:
            r = m - applied * (1.0 / centre)
            alpha = weights[1] * weights[0] / centre
        else:
            r = R[at] - applied
            alpha = weights[step + 1] * weights[step] if step + 1 < ITERS else 0.0
        if step + 1 == ITERS:
            sums[slot] = sums[slot] + r * r
            return [(res, out, r)]
        d = alpha * m + (2.0 * weights[step + 1] / half_width) * r
        s = (m * (1.0 / centre) if step == 0 else S[at]) + d
        return [
            (R, at, r),
            (new, (x, t, pl.ds(row, 8), slice(None)), d),
            (S, at, s) if step + 2 < ITERS else (sol, out, s),
        ]

    def late(parts):
        held = []
        for part in parts:
            stores = part()
            for ref, at, value in held:
                ref[at] = value
            held = stores
        for ref, at, value in held:
            ref[at] = value

    def groups(step, items, halo, sums=None):
        late([functools.partial(row_group, step, x, j, range(NT), halo, sums) for x, j in items])

    def layers(step, first, count, js, halo, many, sums):
        def body(i, carry):
            part = list(carry)
            groups(step, [(first + i * many + k, j) for k in range(many) for j in js], halo, part)
            return tuple(part)

        sums[:] = lax.fori_loop(0, count // many, body, tuple(sums))

    def faces(step, t, sums):
        cur, new, more = step % 2, (step + 1) % 2, step + 1 < ITERS
        for h in range(NH):
            x_each(cur, t, h, "wait_recv")
            if h == 0:
                y_each(cur, t + 1, "wait_recv", (1,))
            if h == NH - 1:
                y_each(cur, t + 1, "wait_recv", (0,))
            js = range(h * (NJ // NH), (h + 1) * (NJ // NH))
            halo = ZH[cur, 1] if isinstance(t, int) else None
            late([functools.partial(face_group, step, x, j, t, halo, sums) for j in js for x in (1, NXL)])
            if more:
                x_each(new, t, h, "start")
                if h == 0:
                    y_each(new, t + 1, "start", (0,))
                if h == NH - 1:
                    y_each(new, t + 1, "start", (1,))

    for t, h in chunks:
        x_each(0, t, h, "start")
    for copy in rest:
        copy.wait()
    for chunk in range(NT + 1):
        y_each(0, chunk, "start")
    for part in range(3):
        z_pack(0, part)
        z_copy(0, part).start()

    for step in range(ITERS):
        cur, new, more = step % 2, (step + 1) % 2, step + 1 < ITERS
        y_each(cur, 0, "wait_recv")
        z_copy(cur, 0).wait_recv()
        halo = ZH[cur, 0]
        sums = [] if more else [jnp.zeros((8, 128), F32)] * NT
        if step == 0:
            for copy in slabs[0] + slabs[1] + slabs[2]:
                copy.wait()
            layers(step, 2, 4, range(NJ), halo, 2, sums)
            for copy in slabs[3]:
                copy.wait()
            layers(step, 6, 4, range(NJ), halo, 2, sums)
            for copy in slabs[4]:
                copy.wait()
            layers(step, 10, 6, (0, NJ - 1), halo, 6, sums)
            y_each(new, 0, "start")
        else:
            layers(step, 2, NXL - 2, (0, NJ - 1), halo, 7, sums)
            if more:
                y_each(new, 0, "start")
            layers(step, 2, 8, middle, halo, 2, sums)
        if more:
            z_pack(new, 0)
            z_copy(new, 0).start()
        def face_tile(t, carry):
            part = list(carry)
            faces(step, t, part)
            pl.when(t == 0)(lambda: z_copy(cur, 2).wait_recv())
            groups(step, [(10 + 2 * t + k, j) for k in range(2) for j in middle], ZH[cur, 2], part)
            return tuple(part)

        sums = list(lax.fori_loop(0, NT - 1, face_tile, tuple(sums)))
        if more:
            z_pack(new, 2)
            z_copy(new, 2).start()
        z_copy(cur, 1).wait_recv()
        faces(step, NT - 1, sums)
        if more:
            z_pack(new, 1)
            z_copy(new, 1).start()
            for t, h in chunks:
                x_each(cur, t, h, "wait_send")
            for chunk in range(NT + 1):
                y_each(cur, chunk, "wait_send")
            for part in range(3):
                z_copy(cur, part).wait_send()
    total = jnp.sum((sums[0] + sums[1]) + (sums[2] + sums[3]), axis=0, keepdims=True)

    def stage(total, G, send, recv, own, count, place, order, meanwhile):
        G[own, pl.ds(0, 1), :] = total
        copies = [
            pltpu.make_async_remote_copy(
                src_ref=G.at[own, pl.ds(0, 1), :],
                dst_ref=G.at[own, pl.ds(0, 1), :],
                send_sem=send.at[o - 1],
                recv_sem=recv.at[o - 1],
                device_id=place((own + o) % count),
                device_id_type=MESH,
            )
            for o in order
        ]
        for copy in copies:
            copy.start()
        meanwhile()
        for copy in copies:
            copy.wait_recv()
        parts = [G[i, pl.ds(0, 1), :] for i in range(count)]
        while len(parts) > 1:
            parts = [a + b for a, b in zip(parts[::2], parts[1::2])]
        return parts[0], copies

    def last_sends():
        cur = (ITERS - 1) % 2
        for t, h in chunks:
            x_each(cur, t, h, "wait_send")
        for chunk in range(NT + 1):
            y_each(cur, chunk, "wait_send")
        for part in range(3):
            z_copy(cur, part).wait_send()

    far_first = (10, 6, 9, 11, 7, 5, 2, 14, 8, 3, 13, 1, 15, 4, 12)
    total, c1 = stage(total, G1, g1s, g1r, gx, 16, lambda p: (p, gy, gz), far_first, last_sends)
    total, c2 = stage(total, G2, g2s, g2r, yz, 8, lambda p: (gx, p // 2, p % 2), range(1, 8), lambda: None)
    whole = jnp.sum(total, axis=1, keepdims=True)
    norm[...] = jnp.sqrt(whole * (1.0 / CELLS) + 1e-06)
    for copy in c1 + c2:
        copy.wait_send()


def local(right_side, reaction, velocity):
    sem = pltpu.SemaphoreType.DMA
    shape = right_side.shape
    sol, res, norm = pl.pallas_call(
        kernel,
        name="chebyshev",
        out_shape=(pltpu.VMEM(shape, F32), pltpu.VMEM(shape, F32), jax.ShapeDtypeStruct((1, 1), F32)),
        in_specs=[pl.BlockSpec(memory_space=pltpu.HBM)] * 3,
        out_specs=(pl.BlockSpec(memory_space=pltpu.VMEM),) * 3,
        scratch_shapes=[
            pltpu.VMEM((NXL + 2, NT, NYL + 16, 128), F32),
            pltpu.VMEM((NXL + 2, NT, NYL + 16, 128), F32),
            pltpu.VMEM((NXL, NT, NYL, 128), F32),
            pltpu.VMEM((NXL, NT, NYL, 128), F32),
            pltpu.VMEM((3, NXL, NT, NYL, 128), F32),
            pltpu.VMEM((NXL, NT, NYL, 128), F32),
            pltpu.VMEM((2, 3, 8, 128), F32),
            pltpu.VMEM((2, 3, 8, 128), F32),
            pltpu.VMEM((16, 8, 128), F32),
            pltpu.VMEM((8, 8, 128), F32),
            sem((2, NT)), sem((NT,)), sem((5, NT)), sem((5, 3, NT)),
            sem((2, 2, NT, NH)), sem((2, 2, NT, NH)), sem((2, 2, NT + 1, 2)), sem((2, 2, NT + 1, 2)),
            sem((2, 3)), sem((2, 3)), sem((15,)), sem((15,)), sem((7,)), sem((7,)),
        ],
        compiler_params=pltpu.CompilerParams(
            collective_id=0, has_side_effects=True, vmem_limit_bytes=24 * 1024 * 1024
        ),
    )(*[pltpu.with_memory_space_constraint(a, pltpu.HBM) for a in (right_side, reaction, velocity)])
    return sol, res, norm.reshape(())


def solution(mesh):
    spec = P("gx", "gy", "gz")
    return jax.shard_map(
        local,
        mesh=mesh,
        in_specs=(spec, spec, P(None, "gx", "gy", "gz")),
        out_specs=(spec, spec, P()),
        check_vma=False,
    )
```
